32 devices in a mesh: ctx: 8 (over z, y), tp: 4 (over x, core).
Axes of the slice: x: 2, y: 2, z: 4, core: 2. Of those that a mesh axis runs over, the one named last changes fastest.
Arguments:
- queries: bfloat16 [4096, 4096], P('ctx', 'tp'), may hold values from -22 to 22
- keys: bfloat16 [4096, 512], P('ctx', 'tp'), may hold values from -22 to 22
- values: bfloat16 [4096, 512], P('ctx', 'tp'), may hold values from -36 to 36
- positions: int32 [3, 4096], P(None, 'ctx'), may hold values from 0 to 4095
- segment_ids: int32 [4096], replicated, may hold values from 0 to 3, never falling along the last dimension, each value on 1 to 2048 neighbouring positions
- out_weight: bfloat16 [4096, 8192], P('tp', 'ctx'), may hold values from -0.09375 to 0.09375
- residual: bfloat16 [4096, 8192], P(('ctx', 'tp')), may hold values from -3 to 3
Outputs:
- layer_out: bfloat16 [4096, 8192], P(('ctx', 'tp'))
The draws below stay inside these ranges and needn't reach their ends.
Inputs may be any that keep to these rules, and one draw needn't show every extreme that they name: `segment_ids`: ids never fall along the sequence; each document has 1 to 2048 tokens, and one has exactly 2048.
All inputs are finite; a program needn't handle non-finite values.
Results may differ from the reference program's by a relative error of at most 0.013.
Values may be sent and summed in bfloat16 or wider, within the bound.
A program may use at most 128 MiB of HBM per device.

```python
import math
import jax
import jax.numpy as jnp
import numpy as np
from jax import lax

D = 8192
HD = 128
HQ = 32
HK = 4
DOC = 2048
SEQ = 4096
DOCS = 4
N_TP = 4


def drawn_rows(key, row_count, col_count):
    base_key = jax.random.fold_in(key, 0)
    return jnp.clip(jax.random.normal(base_key, (row_count, col_count), jnp.float32), -6.0, 6.0)


def draw_queries(key, part):
    return drawn_rows(jax.random.fold_in(key, 11), SEQ, HQ * HD).astype(jnp.bfloat16)


def draw_keys(key, part):
    return drawn_rows(jax.random.fold_in(key, 23), SEQ, HK * HD).astype(jnp.bfloat16)


def plant(drawn, stream_key, least, largest):
    index_at = [jax.random.randint(jax.random.fold_in(stream_key, axis), (), 0, length) for axis, length in enumerate(drawn.shape)]
    main_axis = drawn.shape.index(max(drawn.shape))
    beside = index_at[:main_axis] + [(index_at[main_axis] + 1) % drawn.shape[main_axis]] + index_at[main_axis + 1:]
    return drawn.at[tuple(index_at)].set(least).at[tuple(beside)].set(largest)


def levels(key, extent, cuts, least, largest):
    gain = 1.0
    for dim, parts in cuts:
        steps = jax.random.uniform(jax.random.fold_in(jax.random.fold_in(key, 6), dim), (parts,), jnp.float32, least / len(cuts), largest / len(cuts))
        gain = gain * jnp.repeat(jnp.exp(steps), extent[dim] // parts).reshape((-1,) + (1,) * (len(extent) - 1 - dim))
    return gain


def length_profile(count, total, reach, lean):
    portions = [(1 << 20) // math.isqrt(grade ** lean) + 1 for grade in range(2, count + 1)]
    surplus, counts = total - reach - (count - 1), [1] * (count - 1)
    while surplus > 0:
        movable = [i for i in range(count - 1) if counts[i] < reach]
        mass, remaining = sum([portions[i] for i in movable]), surplus
        for i in movable:
            extra = min(reach - counts[i], max(1, remaining * portions[i] // mass), surplus)
            counts[i] = counts[i] + extra
            surplus = surplus - extra
    return np.array([reach] + counts)


def uneven(stream_key, number_of, total, bound, skew):
    if number_of == 2:
        one = jax.random.randint(stream_key, (), max(1, total - bound), min(bound, total - 1) + 1)
        return jnp.stack([one, total - one])
    sizes = jnp.asarray(length_profile(number_of, total, bound, skew), jnp.int32)
    couples = (number_of - 1) // 2
    source_of, receiver = sizes[1:1 + 2 * couples:2], sizes[2:2 + 2 * couples:2]
    margin = jnp.minimum(source_of - 1, bound - receiver)
    moved = jax.random.randint(jax.random.fold_in(stream_key, 1), (couples,), 0, 1 << 20) % (margin + 1)
    sizes = sizes.at[1:1 + 2 * couples:2].set(source_of - moved).at[2:2 + 2 * couples:2].set(receiver + moved)
    return sizes[jax.random.permutation(jax.random.fold_in(stream_key, 2), number_of)]


def noise(stream_key, shape, scale, limit, shards=(), kind=jnp.bfloat16):
    array = jax.random.normal(stream_key, shape, jnp.float32) * scale
    if len(shards) > 0:
        array = levels(stream_key, shape, shards, -0.22, 0.18) * array
    return jnp.clip(array, min=-limit, max=limit).astype(kind)


def setup_inputs(seed: int = 0) -> dict:
    seeds = jax.random.split(jax.random.key(seed), 8)
    return {
        "queries": draw_queries(jax.random.fold_in(seeds[7], 71), 0),
        "keys": draw_keys(jax.random.fold_in(seeds[7], 71), 0),
        "values": noise(seeds[2], (SEQ, HK * HD), 6.0, 36.0, ((0, 8), (1, 4))),
        "positions": plant(jax.random.randint(seeds[3], (3, SEQ), 0, SEQ), jax.random.fold_in(seeds[3], 1), 0, SEQ - 1).astype(jnp.int32),
        "segment_ids": jnp.searchsorted(jnp.cumsum(uneven(seeds[4], DOCS, SEQ, DOC, 1)), jnp.arange(SEQ), side="right").astype(jnp.int32),
        "out_weight": noise(seeds[5], (HQ * HD, D), (HQ * HD) ** -0.5, 0.09375, ((0, 4), (1, 8))),
        "residual": noise(seeds[6], (SEQ, D), 0.5, 3.0, ((0, 32),)),
    }


theta_base = 1000000.0

def rotary_tables(positions):
    half_dim = HD // 2
    freq_index = jnp.arange(half_dim)
    inv_freq = theta_base ** (-2.0 * freq_index.astype(jnp.float32) / HD)
    first_end = HD // 8
    second_end = first_end + 3 * HD // 16
    place = positions.astype(jnp.float32)
    chosen = jnp.where(freq_index[None, :] < first_end, place[0][:, None], jnp.where(freq_index[None, :] < second_end, place[1][:, None], place[2][:, None]))
    angle = chosen * inv_freq[None, :]
    return (jnp.cos(angle), jnp.sin(angle))

def rotate(vectors, cosine_table, sine_table):
    half_dim = HD // 2
    lower_half = vectors[..., :half_dim]
    upper_half = vectors[..., half_dim:]
    cos_b = cosine_table[:, None, :]
    sin_b = sine_table[:, None, :]
    return jnp.concatenate([lower_half * cos_b - upper_half * sin_b, upper_half * cos_b + lower_half * sin_b], axis=-1)

def reference(queries, keys, values, positions, segment_ids, out_weight, residual):
    seq_len = queries.shape[0]
    group_size = HQ // HK
    cosine_table, sine_table = rotary_tables(positions)
    rot_q = rotate(queries.reshape(seq_len, HQ, HD).astype(jnp.float32), cosine_table, sine_table).astype(jnp.bfloat16)
    rot_k = rotate(keys.reshape(seq_len, HK, HD).astype(jnp.float32), cosine_table, sine_table).astype(jnp.bfloat16)
    key_heads = rot_k.transpose(1, 0, 2)
    value_heads = values.reshape(seq_len, HK, HD).transpose(1, 0, 2)
    query_rows = math.gcd(seq_len, 512)
    key_span = min(seq_len, DOC + query_rows)
    score_scale = 1.0 / math.sqrt(HD)

    def one_block(block_index):
        begin = (block_index * query_rows).astype(jnp.int32)
        key_start = jnp.clip(begin + query_rows - key_span, 0, seq_len - key_span).astype(jnp.int32)
        query_block = lax.dynamic_slice_in_dim(rot_q, begin, query_rows, 0)
        query_index = begin + jnp.arange(query_rows, dtype=jnp.int32)
        key_index = key_start + jnp.arange(key_span, dtype=jnp.int32)
        query_seg = lax.dynamic_slice_in_dim(segment_ids, begin, query_rows, 0)
        key_seg = lax.dynamic_slice_in_dim(segment_ids, key_start, key_span, 0)
        allowed = (key_index[None, :] <= query_index[:, None]) & (key_seg[None, :] == query_seg[:, None])
        grouped = query_block.reshape(query_rows, HK, group_size, HD).transpose(1, 0, 2, 3)
        key_part = lax.dynamic_slice_in_dim(key_heads, key_start, key_span, 1)
        value_part = lax.dynamic_slice_in_dim(value_heads, key_start, key_span, 1)

        def one_head(operands):
            query_head, key_head, value_head = operands
            score = jnp.einsum('qgd,nd->gqn', query_head.astype(jnp.float32), key_head.astype(jnp.float32)) * score_scale
            score = jnp.where(allowed[None], score, -1e+30)
            row_peak = lax.optimization_barrier(jnp.max(score, axis=-1, keepdims=True))
            prob = jnp.where(allowed[None], jnp.exp(score - row_peak), 0.0)
            row_sum = lax.optimization_barrier(jnp.sum(prob, axis=-1))
            mixed = jnp.einsum('gqn,nd->gqd', prob.astype(jnp.bfloat16).astype(jnp.float32), value_head.astype(jnp.float32))
            return (mixed / row_sum[..., None]).transpose(1, 0, 2)
        heads_out = lax.map(one_head, (grouped, key_part, value_part))
        return heads_out.transpose(1, 0, 2, 3).reshape(query_rows, HQ * HD)
    blocks = lax.map(one_block, jnp.arange(seq_len // query_rows, dtype=jnp.int32))
    attended = blocks.reshape(seq_len, HQ * HD).astype(jnp.bfloat16)
    part_cols = HQ * HD // N_TP
    summed = residual.astype(jnp.float32)
    for part_index in range(N_TP):
        cols = attended[:, part_index * part_cols:(part_index + 1) * part_cols]
        rows_w = out_weight[part_index * part_cols:(part_index + 1) * part_cols]
        partial_sum = jnp.dot(cols, rows_w, preferred_element_type=jnp.float32).astype(jnp.bfloat16)
        summed = summed + partial_sum.astype(jnp.float32)
    return summed.astype(jnp.bfloat16)
```

```python
import functools
import math

import jax
import jax.numpy as jnp
from jax import lax
from jax.experimental import pallas as pl
from jax.experimental.pallas import tpu as pltpu
from jax.sharding import PartitionSpec as P

HD = 128
DOC = 2048

theta_base = 1000000.0
MESH_ID = pl.DeviceIdType.MESH


def rotary_tables(positions):
    half_dim = HD // 2
    freq_index = jnp.arange(half_dim)
    inv_freq = theta_base ** (-2.0 * freq_index.astype(jnp.float32) / HD)
    first_end = HD // 8
    second_end = first_end + 3 * HD // 16
    place = positions.astype(jnp.float32)
    chosen = jnp.where(
        freq_index[None, :] < first_end,
        place[0][:, None],
        jnp.where(freq_index[None, :] < second_end, place[1][:, None], place[2][:, None]),
    )
    angle = chosen * inv_freq[None, :]
    return (jnp.cos(angle), jnp.sin(angle))


def rotate(vectors, cosine_table, sine_table):
    half_dim = HD // 2
    lower_half = vectors[..., :half_dim]
    upper_half = vectors[..., half_dim:]
    cos_b = cosine_table[:, None, :]
    sin_b = sine_table[:, None, :]
    return jnp.concatenate(
        [lower_half * cos_b - upper_half * sin_b, upper_half * cos_b + lower_half * sin_b], axis=-1
    )


def fused(
    n, inner, reach, tile,
    q_ref, kv_ref, start_ref, w_ref, out_ref,
    kvbuf, wbuf, att, abuf, bias, pbuf, hbuf, xrecv, obuf,
    kv_s, kv_r, w_r, wu_s, wd_s, wm_s, a_s, a_r, ha_s, ha_r, x_s, x_r, p_s, p_r, o_s, o_r,
):
    outer = n // inner
    tok = q_ref.shape[0]
    pairs = q_ref.shape[1] // (2 * HD)
    tiles = tok // tile
    span = reach * tok + tile
    quarter = tok // 4
    pieces, cut = wbuf.shape[2], wbuf.shape[4]
    cols = w_ref.shape[1]
    block = inner * quarter
    chained = reach % inner == 0
    c = lax.axis_index("ctx")
    t = lax.axis_index("tp")
    co, ci = c // inner, c % inner
    x, h = t // 2, t % 2
    other_x = 1 - x
    last = outer - 1
    is_end = (co == 0) | (co == last)
    helps = (co == 1) | (co == last - 1)
    helped = jnp.where(co == 1, 0, last)
    helper = jnp.where(co == 0, 1, last - 1)
    mate = {"ctx": c, "tp": 2 * x + 1 - h}
    across = {"ctx": c, "tp": 2 * other_x + h}

    def remote(src, dst, send, recv, device):
        return pltpu.make_async_remote_copy(
            src_ref=src, dst_ref=dst, send_sem=send, recv_sem=recv,
            device_id=device, device_id_type=MESH_ID,
        )

    def landed(dst, sem):
        pltpu.make_async_copy(dst, dst, sem).wait()

    def own_piece(j):
        return pltpu.make_async_copy(
            w_ref.at[:, j * cut:(j + 1) * cut], wbuf.at[co, h, j], w_r.at[co, h, j]
        )

    for j in range(pieces):
        own_piece(j).start()

    barrier = pltpu.get_barrier_semaphore()

    def greet(device):
        pl.semaphore_signal(barrier, inc=1, device_id=device, device_id_type=MESH_ID)

    for k in range(inner):
        near = (ci + k) % inner
        for g in range(2):
            if k + g > 0:
                greet({"ctx": co * inner + near, "tp": 2 * x + (h + g) % 2})

            @pl.when(co < last)
            def _():
                greet({"ctx": (co + 1) * inner + near, "tp": 2 * x + g})

            @pl.when(co > 0)
            def _():
                greet({"ctx": (co - 1) * inner + near, "tp": 2 * x + g})
    greet(across)
    beside = jnp.where(co < last, 1, 0) + jnp.where(co > 0, 1, 0)
    pl.semaphore_wait(barrier, 2 * inner + 2 * inner * beside)

    def kv_slot(d):
        start = (reach - d) * tok
        if not isinstance(d, int):
            start = pl.multiple_of(start, tok)
        return kvbuf.at[:, pl.ds(start, tok), :]

    def kv_sends(s, action):
        src = kv_ref if s == 0 else kv_slot(s * inner)

        def one(k, slot, device):
            action(remote(src, kv_slot(slot), kv_s.at[s, k], kv_r.at[slot - 1], device))

        if not chained:
            for d in range(1, reach + 1):
                @pl.when(c + d < n)
                def _():
                    one(d, d, {"ctx": c + d, "tp": t})
            return

        @pl.when(co >= s)
        def _():
            if (s + 1) * inner <= reach:
                @pl.when(co < last)
                def _():
                    one(0, (s + 1) * inner, {"ctx": c + inner, "tp": t})
            for k in range(1, inner):
                near = (ci + k) % inner
                away = s * inner + near - ci

                @pl.when((away >= 1) & (away <= reach))
                def _():
                    one(k, away, {"ctx": co * inner + near, "tp": t})

    stages = reach // inner + 1 if chained else 1
    kv_sends(0, lambda copy: copy.start())

    def w_up(slot, j):
        device = {"ctx": c + inner, "tp": t}
        return remote(wbuf.at[slot, h, j], wbuf.at[slot, h, j], wu_s.at[slot, j], w_r.at[slot, h, j], device)

    def w_down(slot, j):
        device = {"ctx": c - inner, "tp": t}
        return remote(wbuf.at[slot, h, j], wbuf.at[slot, h, j], wd_s.at[slot, j], w_r.at[slot, h, j], device)

    def w_mate(slot, j):
        return remote(wbuf.at[slot, h, j], wbuf.at[slot, h, j], wm_s.at[slot, j], w_r.at[slot, h, j], mate)

    def goes_up(slot):
        return (slot <= co) & (co < last) & ((co + 1 < last) | (slot == co))

    def goes_down(slot):
        return (slot >= co) & (co > 0) & ((co > 1) | (slot == co))

    def has(slot):
        return jnp.logical_not(is_end) | ((slot - co <= 1) & (co - slot <= 1))

    def pass_on(slot, j):
        @pl.when(goes_up(slot))
        def _():
            w_up(slot, j).start()

        @pl.when(goes_down(slot))
        def _():
            w_down(slot, j).start()

        w_mate(slot, j).start()

    early = min(2, pieces)
    own_piece(0).wait()
    pass_on(co, 0)

    kvbuf[:, reach * tok:, :] = kv_ref[...]
    for d in range(1, reach + 1):
        @pl.when(c < d)
        def _():
            kvbuf[:, (reach - d) * tok:(reach - d + 1) * tok, :] = jnp.zeros(kv_ref.shape, kv_ref.dtype)

    def fill_bias(rt, _):
        first = start_ref[pl.ds(pl.multiple_of(rt * tile, tile), tile), :] - (
            (c - reach) * tok + rt * tile
        )
        key = lax.broadcasted_iota(jnp.int32, (tile, span), 1)
        query = lax.broadcasted_iota(jnp.int32, (tile, span), 0) + reach * tok
        bias[rt] = jnp.where((key <= query) & (key >= first), 0.0, -1e30).astype(jnp.float32)
        return 0

    lax.fori_loop(0, tiles, fill_bias, 0)

    for s in range(1, stages):
        @pl.when(co >= s)
        def _():
            landed(kv_slot(s * inner), kv_r.at[s * inner - 1])

        kv_sends(s, lambda copy: copy.start())

    for j in range(1, pieces):
        own_piece(j).wait()
        if j < early:
            pass_on(co, j)
        else:
            @pl.when(jnp.logical_not(is_end))
            def _():
                pass_on(co, j)

    for d in range(1, reach + 1):
        if not chained or d % inner != 0:
            @pl.when(c >= d)
            def _():
                landed(kv_slot(d), kv_r.at[d - 1])

    factor = math.log2(math.e) / math.sqrt(HD)

    def rows_of(side, at):
        return pl.ds(pl.multiple_of((side * inner + at) * quarter, quarter), quarter)

    def a_copies(hp, action):
        lanes = pl.ds(pl.multiple_of(hp * 2 * HD, 2 * HD), 2 * HD)
        for side in range(2):
            for k in range(inner):
                near = (ci + k) % inner
                for gg in range(2):
                    g = (h + gg) % 2
                    src = att.at[pl.ds(pl.multiple_of((2 * side + g) * quarter, quarter), quarter), lanes]
                    if k + gg > 0:
                        action(remote(
                            src, abuf.at[0, h, rows_of(side, ci), lanes], a_s.at[k, gg],
                            a_r.at[ci, h, side], {"ctx": co * inner + near, "tp": 2 * x + g},
                        ))

                    @pl.when(is_end)
                    def _():
                        action(remote(
                            src, abuf.at[1, h, rows_of(side, ci), lanes], ha_s.at[k, gg],
                            ha_r.at[ci, h, side], {"ctx": helper * inner + near, "tp": 2 * x + g},
                        ))

    def attend(hp, _):
        lanes = pl.ds(pl.multiple_of(hp * 2 * HD, 2 * HD), 2 * HD)

        def one_tile(rt, _):
            at = pl.ds(pl.multiple_of(rt * tile, tile), tile)
            window = pl.ds(pl.multiple_of(rt * tile, tile), span)
            k = kvbuf[0, window, :]
            v = kvbuf[1, window, :]
            q2 = q_ref[at, lanes]
            done = []
            for e in range(2):
                q = q2[:, e * HD:(e + 1) * HD]
                s = lax.dot_general(
                    q, k, (((1,), (1,)), ((), ())), preferred_element_type=jnp.float32
                ) + bias[rt]
                peak = jnp.max(s, axis=-1, keepdims=True)
                p = jnp.exp2((s - peak) * factor)
                total = jnp.sum(p, axis=-1, keepdims=True)
                mixed = jnp.dot(p.astype(jnp.bfloat16), v, preferred_element_type=jnp.float32)
                done.append((mixed / total).astype(jnp.bfloat16))
            att[at, lanes] = jnp.concatenate(done, axis=1)
            return 0

        lax.fori_loop(0, tiles, one_tile, 0)
        a_copies(hp, lambda copy: copy.start())
        for side in range(2):
            src = pl.ds(pl.multiple_of((2 * side + h) * quarter, quarter), quarter)
            abuf[0, h, rows_of(side, ci), lanes] = att[src, lanes]
        return 0

    lax.fori_loop(0, pairs, attend, 0)

    @pl.when(is_end)
    def _():
        for j in range(early, pieces):
            pass_on(co, j)

    for k in range(inner):
        near = (ci + k) % inner
        for gg in range(2):
            if k + gg > 0:
                g = (h + gg) % 2
                for side in range(2):
                    landed(abuf.at[0, g, rows_of(side, near), :], a_r.at[near, g, side])

    def x_copy(slot, j):
        return remote(pbuf.at[slot, j, other_x], xrecv.at[slot, j], x_s.at[slot, j], x_r.at[slot, j], across)

    def p_copy(slot, j):
        device = {"ctx": helped * inner + ci, "tp": t}
        return remote(hbuf.at[slot, j], pbuf.at[slot, j], p_s.at[slot, j], p_r.at[slot, j], device)

    def out_slot(slot, j, at):
        return out_ref.at[:, pl.ds(pl.multiple_of((slot * inner + at) * cols + j * cut, 128), cut)]

    def o_copy(slot, j, k):
        near = (ci + k) % inner
        device = {"ctx": co * inner + near, "tp": t}
        return remote(obuf.at[slot, j, near], out_slot(slot, j, ci), o_s.at[slot, j, k], o_r.at[slot, j, ci], device)

    def product(who, slot, j, into):
        for side in range(2):
            at = slice(side * block, (side + 1) * block)
            into[slot, j, side] = (
                jnp.dot(abuf[who, 0, at, :], wbuf[slot, 0, j], preferred_element_type=jnp.float32)
                + jnp.dot(abuf[who, 1, at, :], wbuf[slot, 1, j], preferred_element_type=jnp.float32)
            ).astype(jnp.bfloat16)

    def lends(slot):
        return helps & (slot != helped) & (slot != co)

    def send_product(d, slot, j):
        @pl.when(has(slot))
        def _():
            @pl.when(d > 0)
            def _():
                landed(wbuf.at[slot, h, j], w_r.at[slot, h, j])
                pass_on(slot, j)

            landed(wbuf.at[slot, 1 - h, j], w_r.at[slot, 1 - h, j])

            @pl.when(lends(slot))
            def _():
                product(1, slot, j, hbuf)
                p_copy(slot, j).start()

            product(0, slot, j, pbuf)

        @pl.when(jnp.logical_not(has(slot)))
        def _():
            landed(pbuf.at[slot, j], p_r.at[slot, j])

        x_copy(slot, j).start()

    def add_product(slot, j):
        landed(xrecv.at[slot, j], x_r.at[slot, j])
        both = (
            pbuf[slot, j, x].astype(jnp.float32) + xrecv[slot, j].astype(jnp.float32)
        ).astype(jnp.bfloat16)
        for k in range(inner):
            obuf[slot, j, k] = both[k * quarter:(k + 1) * quarter]
        for k in range(1, inner):
            o_copy(slot, j, k).start()
        out_ref[:, pl.ds(pl.multiple_of((slot * inner + ci) * cols + j * cut, 128), cut)] = obuf[slot, j, ci]

    def each_side(distance, action):
        def one_side(side, _):
            slot = co + distance * (2 * side - 1)

            @pl.when((slot >= 0) & (slot < outer) & ((distance > 0) | (side == 1)))
            def _():
                action(slot)
            return 0

        lax.fori_loop(0, 2, one_side, 0)

    def first_unit(j, _):
        send_product(0, co, j)
        return 0

    lax.fori_loop(0, pieces, first_unit, 0)

    @pl.when(helps)
    def _():
        for k in range(inner):
            for g in range(2):
                for side in range(2):
                    landed(abuf.at[1, g, rows_of(side, k), :], ha_r.at[k, g, side])

    def step(i, _):
        d, j = i // pieces, i % pieces

        @pl.when(d < outer)
        def _():
            each_side(d, lambda slot: send_product(d, slot, j))

        before = i - pieces
        each_side(before // pieces, lambda slot: add_product(slot, before % pieces))
        return 0

    lax.fori_loop(pieces, (outer + 1) * pieces, step, 0)

    for s in range(stages):
        kv_sends(s, lambda copy: copy.wait_send())
    for k in range(inner):
        for gg in range(2):
            if k + gg > 0:
                landed(abuf.at[0, 0, 0:2 * quarter, :], a_s.at[k, gg])

            @pl.when(is_end)
            def _():
                landed(abuf.at[0, 0, 0:2 * quarter, :], ha_s.at[k, gg])

    def drain(i, _):
        slot, j = i // pieces, i % pieces

        @pl.when(has(slot))
        def _():
            w_mate(slot, j).wait_send()

            @pl.when(goes_up(slot))
            def _():
                w_up(slot, j).wait_send()

            @pl.when(goes_down(slot))
            def _():
                w_down(slot, j).wait_send()

        @pl.when(lends(slot))
        def _():
            p_copy(slot, j).wait_send()

        x_copy(slot, j).wait_send()
        for k in range(1, inner):
            o_copy(slot, j, k).wait_send()
            near = (ci + k) % inner
            landed(out_slot(slot, j, near), o_r.at[slot, j, near])
        return 0

    lax.fori_loop(0, outer * pieces, drain, 0)


def on_device(queries, keys, values, positions, segment_ids, out_weight, residual):
    tok = queries.shape[0]
    heads = queries.shape[1] // HD
    n = lax.axis_size("ctx")
    inner = 2 ** max(1, int(math.log2(n)) // 2)
    outer = n // inner
    reach = (DOC + tok - 2) // tok
    tile = math.gcd(tok, 256)
    my_start = lax.axis_index("ctx") * tok
    depth, cols = out_weight.shape
    cut = math.gcd(cols, 256)
    pieces = cols // cut
    cosine_table, sine_table = rotary_tables(positions)
    rot_q = rotate(
        queries.reshape(tok, heads, HD).astype(jnp.float32), cosine_table, sine_table
    ).astype(jnp.bfloat16).reshape(tok, heads * HD)
    rot_k = rotate(
        keys.reshape(tok, 1, HD).astype(jnp.float32), cosine_table, sine_table
    ).astype(jnp.bfloat16).reshape(tok, HD)
    pair = jnp.stack([rot_k, values], axis=0)
    my_seg = lax.dynamic_slice_in_dim(segment_ids, my_start, tok, 0)
    start = jnp.sum((segment_ids[None, :] < my_seg[:, None]).astype(jnp.int32), axis=1, keepdims=True)
    quarter = tok // 4
    block = inner * quarter
    bf16 = jnp.bfloat16
    dma = pltpu.SemaphoreType.DMA
    vmem = pl.BlockSpec(memory_space=pltpu.VMEM)
    gathered = pl.pallas_call(
        functools.partial(fused, n, inner, reach, tile),
        out_shape=jax.ShapeDtypeStruct((quarter, n * cols), bf16),
        in_specs=[vmem] * 3 + [pl.BlockSpec(memory_space=pl.ANY)],
        out_specs=vmem,
        scratch_shapes=[
            pltpu.VMEM((2, (reach + 1) * tok, HD), bf16),
            pltpu.VMEM((outer, 2, pieces, depth, cut), bf16),
            pltpu.VMEM((tok, depth), bf16),
            pltpu.VMEM((2, 2, 2 * block, depth), bf16),
            pltpu.VMEM((tok // tile, tile, reach * tok + tile), jnp.float32),
            pltpu.VMEM((outer, pieces, 2, block, cut), bf16),
            pltpu.VMEM((outer, pieces, 2, block, cut), bf16),
            pltpu.VMEM((outer, pieces, block, cut), bf16),
            pltpu.VMEM((outer, pieces, inner, quarter, cut), bf16),
            dma((reach + 1, max(inner, reach + 1))), dma((reach,)),
            dma((outer, 2, pieces)),
            dma((outer, pieces)), dma((outer, pieces)), dma((outer, pieces)),
            dma((inner, 2)), dma((inner, 2, 2)),
            dma((inner, 2)), dma((inner, 2, 2)),
            dma((outer, pieces)), dma((outer, pieces)),
            dma((outer, pieces)), dma((outer, pieces)),
            dma((outer, pieces, inner)), dma((outer, pieces, inner)),
        ],
        compiler_params=pltpu.CompilerParams(
            collective_id=0, has_side_effects=True, vmem_limit_bytes=60 * 1024 * 1024
        ),
    )(rot_q, pair, start, out_weight)
    return (gathered.astype(jnp.float32) + residual.astype(jnp.float32)).astype(jnp.bfloat16)


def solution(mesh):
    return jax.shard_map(
        on_device,
        mesh=mesh,
        in_specs=(
            P("ctx", "tp"),
            P("ctx", "tp"),
            P("ctx", "tp"),
            P(None, "ctx"),
            P(),
            P("tp", "ctx"),
            P(("ctx", "tp"), None),
        ),
        out_specs=P(("ctx", "tp"), None),
        check_vma=False,
    )
```

```python
import functools
import math

import jax
import jax.numpy as jnp
from jax import lax
from jax.experimental import pallas as pl
from jax.experimental.pallas import tpu as pltpu
from jax.sharding import PartitionSpec as P

HD = 128
DOC = 2048

theta_base = 1000000.0
MESH_ID = pl.DeviceIdType.MESH


def rotary_tables(positions):
    half_dim = HD // 2
    freq_index = jnp.arange(half_dim)
    inv_freq = theta_base ** (-2.0 * freq_index.astype(jnp.float32) / HD)
    first_end = HD // 8
    second_end = first_end + 3 * HD // 16
    place = positions.astype(jnp.float32)
    chosen = jnp.where(
        freq_index[None, :] < first_end,
        place[0][:, None],
        jnp.where(freq_index[None, :] < second_end, place[1][:, None], place[2][:, None]),
    )
    angle = chosen * inv_freq[None, :]
    return (jnp.cos(angle), jnp.sin(angle))


def rotate(vectors, cosine_table, sine_table):
    half_dim = HD // 2
    lower_half = vectors[..., :half_dim]
    upper_half = vectors[..., half_dim:]
    cos_b = cosine_table[:, None, :]
    sin_b = sine_table[:, None, :]
    return jnp.concatenate(
        [lower_half * cos_b - upper_half * sin_b, upper_half * cos_b + lower_half * sin_b], axis=-1
    )


def fused(
    n, inner, reach, tile,
    q_ref, kv_ref, start_ref, w_ref, out_ref,
    kvbuf, wbuf, att, abuf, bias, pbuf, xrecv, obuf,
    kv_s, kv_r, w_r, wu_s, wd_s, wm_s, a_s, a_r, ha_s, hf_s, ha_r, x_s, x_r, o_s, o_r,
):
    outer = n // inner
    tok = q_ref.shape[0]
    pairs = q_ref.shape[1] // (2 * HD)
    tiles = tok // tile
    span = reach * tok + tile
    quarter = tok // 4
    pieces, cut = wbuf.shape[2], wbuf.shape[4]
    cols = w_ref.shape[1]
    block = inner * quarter
    chained = reach % inner == 0
    c = lax.axis_index("ctx")
    t = lax.axis_index("tp")
    co, ci = c // inner, c % inner
    x, h = t // 2, t % 2
    other_x = 1 - x
    last = outer - 1
    is_end = (co == 0) | (co == last)
    helps = (co == 1) | (co == last - 1)
    helped = jnp.where(co == 1, 0, last)
    helper = jnp.where(co == 0, 1, last - 1)
    mate = {"ctx": c, "tp": 2 * x + 1 - h}
    across = {"ctx": c, "tp": 2 * other_x + h}

    def remote(src, dst, send, recv, device):
        return pltpu.make_async_remote_copy(
            src_ref=src, dst_ref=dst, send_sem=send, recv_sem=recv,
            device_id=device, device_id_type=MESH_ID,
        )

    def landed(dst, sem):
        pltpu.make_async_copy(dst, dst, sem).wait()

    def own_piece(j):
        return pltpu.make_async_copy(
            w_ref.at[:, j * cut:(j + 1) * cut], wbuf.at[co, h, j], w_r.at[co, h, j]
        )

    for j in range(pieces):
        own_piece(j).start()

    barrier = pltpu.get_barrier_semaphore()

    def greet(device):
        pl.semaphore_signal(barrier, inc=1, device_id=device, device_id_type=MESH_ID)

    for k in range(inner):
        near = (ci + k) % inner
        for g in range(2):
            if k + g > 0:
                greet({"ctx": co * inner + near, "tp": 2 * x + (h + g) % 2})

            @pl.when(co < last)
            def _():
                greet({"ctx": (co + 1) * inner + near, "tp": 2 * x + g})

            @pl.when(co > 0)
            def _():
                greet({"ctx": (co - 1) * inner + near, "tp": 2 * x + g})
    greet(across)
    beside = jnp.where(co < last, 1, 0) + jnp.where(co > 0, 1, 0)
    pl.semaphore_wait(barrier, 2 * inner + 2 * inner * beside)

    half = tok // 2
    kv_parts = 4

    def kv_slot(d, part):
        start = pl.multiple_of((reach - d) * tok + part % 2 * half, half)
        return kvbuf.at[part // 2, pl.ds(start, half), :]

    def kv_sends(s, part, action):
        src = kv_ref.at[part // 2, pl.ds(part % 2 * half, half), :] if s == 0 else kv_slot(s * inner, part)

        def one(k, slot, device):
            action(remote(src, kv_slot(slot, part), kv_s.at[s, k, part], kv_r.at[slot - 1, part], device))

        if not chained:
            for d in range(1, reach + 1):
                @pl.when(c + d < n)
                def _():
                    one(d, d, {"ctx": c + d, "tp": t})
            return

        @pl.when(co >= s)
        def _():
            if (s + 1) * inner <= reach:
                @pl.when(co < last)
                def _():
                    one(0, (s + 1) * inner, {"ctx": c + inner, "tp": t})
            for k in range(1, inner):
                near = (ci + k) % inner
                away = s * inner + near - ci

                @pl.when((away >= 1) & (away <= reach))
                def _():
                    one(k, away, {"ctx": co * inner + near, "tp": t})

    stages = reach // inner + 1 if chained else 1
    for part in range(kv_parts):
        kv_sends(0, part, lambda copy: copy.start())

    early = min(2, pieces)
    shared = pieces // 2

    def w_up(slot, j):
        device = {"ctx": c + inner, "tp": t}
        return remote(wbuf.at[slot, h, j], wbuf.at[slot, h, j], wu_s.at[slot, j], w_r.at[slot, h, j], device)

    def w_down(slot, j):
        device = {"ctx": c - inner, "tp": t}
        return remote(wbuf.at[slot, h, j], wbuf.at[slot, h, j], wd_s.at[slot, j], w_r.at[slot, h, j], device)

    def w_mate(slot, j):
        return remote(wbuf.at[slot, h, j], wbuf.at[slot, h, j], wm_s.at[slot, j], w_r.at[slot, h, j], mate)

    def near_end(away, j):
        return (away <= 1) | ((away == 2) & (j < shared))

    def goes_up(slot, j):
        return (slot <= co) & (co < last) & ((co + 1 < last) | near_end(co + 1 - slot, j))

    def goes_down(slot, j):
        return (slot >= co) & (co > 0) & ((co > 1) | near_end(slot - co + 1, j))

    def has(slot, j):
        return jnp.logical_not(is_end) | (near_end(slot - co, j) & near_end(co - slot, j))

    def lends(slot, j):
        away = jnp.where(slot < helped, helped - slot, slot - helped)
        return helps & jnp.logical_not(near_end(away, j))

    def pass_up(slot, j):
        @pl.when(goes_up(slot, j))
        def _():
            w_up(slot, j).start()

    def pass_down(slot, j):
        @pl.when(goes_down(slot, j))
        def _():
            w_down(slot, j).start()

    def own_up():
        for j in range(pieces):
            if j < early:
                pass_up(co, j)
            else:
                @pl.when(jnp.logical_not(is_end))
                def _():
                    pass_up(co, j)

    for j in range(pieces):
        own_piece(j).wait()
        if j < early:
            pass_down(co, j)
        else:
            @pl.when(jnp.logical_not(is_end))
            def _():
                pass_down(co, j)
        w_mate(co, j).start()

    @pl.when(co == 0)
    def _():
        own_up()

    kvbuf[:, reach * tok:, :] = kv_ref[...]
    for d in range(1, reach + 1):
        @pl.when(c < d)
        def _():
            kvbuf[:, (reach - d) * tok:(reach - d + 1) * tok, :] = jnp.zeros(kv_ref.shape, kv_ref.dtype)

    def fill_bias(rt, _):
        first = start_ref[pl.ds(pl.multiple_of(rt * tile, tile), tile), :] - (
            (c - reach) * tok + rt * tile
        )
        key = lax.broadcasted_iota(jnp.int32, (tile, span), 1)
        query = lax.broadcasted_iota(jnp.int32, (tile, span), 0) + reach * tok
        bias[rt] = jnp.where((key <= query) & (key >= first), 0.0, -1e30).astype(jnp.float32)
        return 0

    lax.fori_loop(0, tiles, fill_bias, 0)

    for s in range(1, stages):
        for part in range(kv_parts):
            @pl.when(co >= s)
            def _():
                landed(kv_slot(s * inner, part), kv_r.at[s * inner - 1, part])

            kv_sends(s, part, lambda copy: copy.start())
        if s == 1:
            @pl.when(co > 0)
            def _():
                own_up()

    if stages == 1:
        @pl.when(co > 0)
        def _():
            own_up()

    for d in range(1, reach + 1):
        if not chained or d % inner != 0:
            @pl.when(c >= d)
            def _():
                for part in range(kv_parts):
                    landed(kv_slot(d, part), kv_r.at[d - 1, part])

    factor = math.log2(math.e) / math.sqrt(HD)

    def rows_of(side, at):
        return pl.ds(pl.multiple_of((side * inner + at) * quarter, quarter), quarter)

    def a_copies(hp, action):
        lanes = pl.ds(pl.multiple_of(hp * 2 * HD, 2 * HD), 2 * HD)
        for side in range(2):
            for k in range(inner):
                near = (ci + k) % inner
                for gg in range(2):
                    g = (h + gg) % 2
                    src = att.at[pl.ds(pl.multiple_of((2 * side + g) * quarter, quarter), quarter), lanes]
                    if k + gg > 0:
                        action(remote(
                            src, abuf.at[0, h, rows_of(side, ci), lanes], a_s.at[k, gg],
                            a_r.at[ci, h, side], {"ctx": co * inner + near, "tp": 2 * x + g},
                        ))

                    if k == 0:
                        @pl.when(is_end)
                        def _():
                            action(remote(
                                src, abuf.at[1, h, rows_of(side, ci), lanes], ha_s.at[gg],
                                ha_r.at[ci, h, side], {"ctx": helper * inner + ci, "tp": 2 * x + g},
                            ))

    def attend(hp, _):
        lanes = pl.ds(pl.multiple_of(hp * 2 * HD, 2 * HD), 2 * HD)

        def one_tile(rt, _):
            at = pl.ds(pl.multiple_of(rt * tile, tile), tile)
            window = pl.ds(pl.multiple_of(rt * tile, tile), span)
            k = kvbuf[0, window, :]
            v = kvbuf[1, window, :]
            q2 = q_ref[at, lanes]
            done = []
            for e in range(2):
                q = q2[:, e * HD:(e + 1) * HD]
                s = lax.dot_general(
                    q, k, (((1,), (1,)), ((), ())), preferred_element_type=jnp.float32
                ) + bias[rt]
                peak = jnp.max(s, axis=-1, keepdims=True)
                p = jnp.exp2((s - peak) * factor)
                total = jnp.sum(p, axis=-1, keepdims=True)
                mixed = jnp.dot(p.astype(jnp.bfloat16), v, preferred_element_type=jnp.float32)
                done.append((mixed / total).astype(jnp.bfloat16))
            att[at, lanes] = jnp.concatenate(done, axis=1)
            return 0

        lax.fori_loop(0, tiles, one_tile, 0)
        a_copies(hp, lambda copy: copy.start())
        for side in range(2):
            src = pl.ds(pl.multiple_of((2 * side + h) * quarter, quarter), quarter)
            abuf[0, h, rows_of(side, ci), lanes] = att[src, lanes]
        return 0

    lax.fori_loop(0, pairs, attend, 0)

    def each_side(distance, j, action):
        def one_side(side, _):
            slot = co + distance * (2 * side - 1)

            @pl.when((slot >= 0) & (slot < outer) & ((distance > 0) | (side == 1)))
            def _():
                @pl.when(has(slot, j))
                def _():
                    action(slot)
            return 0

        lax.fori_loop(0, 2, one_side, 0)

    def arrive(slot, j):
        landed(wbuf.at[slot, h, j], w_r.at[slot, h, j])
        pass_up(slot, j)
        pass_down(slot, j)
        w_mate(slot, j).start()

    def whole(slot, j):
        landed(wbuf.at[slot, 1 - h, j], w_r.at[slot, 1 - h, j])

    @pl.when(is_end)
    def _():
        for j in range(early, pieces):
            pass_up(co, j)
            pass_down(co, j)

    for j in range(early):
        each_side(1, j, lambda slot: arrive(slot, j))

    for k in range(inner):
        near = (ci + k) % inner
        for gg in range(2):
            if k + gg > 0:
                g = (h + gg) % 2
                for side in range(2):
                    landed(abuf.at[0, g, rows_of(side, near), :], a_r.at[near, g, side])

    def x_copy(who, slot, j):
        return remote(
            pbuf.at[who, slot, j, other_x], xrecv.at[who, slot, j],
            x_s.at[who, slot, j], x_r.at[who, slot, j], across,
        )

    def out_slot(slot, j, at):
        return out_ref.at[:, pl.ds(pl.multiple_of((slot * inner + at) * cols + j * cut, 128), cut)]

    def o_copy(who, slot, j, k):
        near = (ci + k) % inner
        node = helped if who else co
        device = {"ctx": node * inner + near, "tp": t}
        return remote(
            obuf.at[who, slot, j, near], out_slot(slot, j, ci),
            o_s.at[who, slot, j, k], o_r.at[slot, j, ci], device,
        )

    def job(who, slot, j):
        for side in range(2):
            at = slice(side * block, (side + 1) * block)
            pbuf[who, slot, j, side] = (
                jnp.dot(abuf[who, 0, at, :], wbuf[slot, 0, j], preferred_element_type=jnp.float32)
                + jnp.dot(abuf[who, 1, at, :], wbuf[slot, 1, j], preferred_element_type=jnp.float32)
            ).astype(jnp.bfloat16)
        x_copy(who, slot, j).start()

    def finish(who, slot, j):
        landed(xrecv.at[who, slot, j], x_r.at[who, slot, j])
        both = (
            pbuf[who, slot, j, x].astype(jnp.float32) + xrecv[who, slot, j].astype(jnp.float32)
        ).astype(jnp.bfloat16)
        for k in range(inner):
            obuf[who, slot, j, k] = both[k * quarter:(k + 1) * quarter]
        for k in range(1 - who, inner):
            o_copy(who, slot, j, k).start()
        if not who:
            out_ref[:, pl.ds(pl.multiple_of((slot * inner + ci) * cols + j * cut, 128), cut)] = obuf[who, slot, j, ci]

    beyond = 2 * co - helped

    def forwards(action):
        for k in range(1, inner):
            near = (ci + k) % inner
            for g in range(2):
                for side in range(2):
                    here = abuf.at[1, g, rows_of(side, ci), :]
                    action(remote(
                        here, here, hf_s.at[k, g, side], ha_r.at[ci, g, side],
                        {"ctx": co * inner + near, "tp": t},
                    ))

    def step(i, _):
        d, j = i // pieces, i % pieces

        @pl.when((d > 1) & (d < outer))
        def _():
            each_side(d, j, lambda slot: arrive(slot, j))

        @pl.when(helps & (i == 1))
        def _():
            for g in range(2):
                for side in range(2):
                    landed(abuf.at[1, g, rows_of(side, ci), :], ha_r.at[ci, g, side])
            forwards(lambda copy: copy.start())

        @pl.when(helps & (i == 2 * pieces))
        def _():
            for k in range(1, inner):
                near = (ci + k) % inner
                for g in range(2):
                    for side in range(2):
                        landed(abuf.at[1, g, rows_of(side, near), :], ha_r.at[near, g, side])

            def lend(jj, _):
                job(1, beyond, jj)
                return 0

            lax.fori_loop(shared, pieces, lend, 0)

        def begins(slot):
            whole(slot, j)

            @pl.when(lends(slot, j) & (d > 1))
            def _():
                job(1, slot, j)

            job(0, slot, j)

        @pl.when(d < outer)
        def _():
            each_side(d, j, begins)

        before = i - lag
        then = before % pieces

        @pl.when(before >= 0)
        def _():
            def ends(slot):
                @pl.when(lends(slot, then) & (before >= 2 * pieces))
                def _():
                    finish(1, slot, then)

                finish(0, slot, then)

            each_side(before // pieces, then, ends)

        @pl.when(helps & (d == 2) & (j >= shared))
        def _():
            finish(1, beyond, j)

        @pl.when((d == 1) & (j + early < pieces))
        def _():
            each_side(1, j, lambda slot: arrive(slot, j + early))
        return 0

    lag = 3
    lax.fori_loop(0, outer * pieces + lag, step, 0)

    for s in range(stages):
        for part in range(kv_parts):
            kv_sends(s, part, lambda copy: copy.wait_send())
    for k in range(inner):
        for gg in range(2):
            if k + gg > 0:
                landed(abuf.at[0, 0, 0:2 * quarter, :], a_s.at[k, gg])

    @pl.when(is_end)
    def _():
        for gg in range(2):
            landed(abuf.at[0, 0, 0:2 * quarter, :], ha_s.at[gg])

    @pl.when(helps)
    def _():
        forwards(lambda copy: copy.wait_send())

    def drain(i, _):
        slot, j = i // pieces, i % pieces

        @pl.when(has(slot, j))
        def _():
            w_mate(slot, j).wait_send()

            @pl.when(goes_up(slot, j))
            def _():
                w_up(slot, j).wait_send()

            @pl.when(goes_down(slot, j))
            def _():
                w_down(slot, j).wait_send()

            x_copy(0, slot, j).wait_send()
            for k in range(1, inner):
                o_copy(0, slot, j, k).wait_send()

        @pl.when(lends(slot, j))
        def _():
            x_copy(1, slot, j).wait_send()
            for k in range(inner):
                o_copy(1, slot, j, k).wait_send()

        for k in range(inner):
            near = (ci + k) % inner
            if k == 0:
                @pl.when(jnp.logical_not(has(slot, j)))
                def _():
                    landed(out_slot(slot, j, near), o_r.at[slot, j, near])
            else:
                landed(out_slot(slot, j, near), o_r.at[slot, j, near])
        return 0

    lax.fori_loop(0, outer * pieces, drain, 0)


def on_device(queries, keys, values, positions, segment_ids, out_weight, residual):
    tok = queries.shape[0]
    heads = queries.shape[1] // HD
    n = lax.axis_size("ctx")
    inner = 2 ** max(1, int(math.log2(n)) // 2)
    outer = n // inner
    reach = (DOC + tok - 2) // tok
    tile = math.gcd(tok, 256)
    my_start = lax.axis_index("ctx") * tok
    depth, cols = out_weight.shape
    cut = math.gcd(cols, 256)
    pieces = cols // cut
    cosine_table, sine_table = rotary_tables(positions)
    rot_q = rotate(
        queries.reshape(tok, heads, HD).astype(jnp.float32), cosine_table, sine_table
    ).astype(jnp.bfloat16).reshape(tok, heads * HD)
    rot_k = rotate(
        keys.reshape(tok, 1, HD).astype(jnp.float32), cosine_table, sine_table
    ).astype(jnp.bfloat16).reshape(tok, HD)
    pair = jnp.stack([rot_k, values], axis=0)
    my_seg = lax.dynamic_slice_in_dim(segment_ids, my_start, tok, 0)
    start = jnp.sum((segment_ids[None, :] < my_seg[:, None]).astype(jnp.int32), axis=1, keepdims=True)
    quarter = tok // 4
    block = inner * quarter
    bf16 = jnp.bfloat16
    dma = pltpu.SemaphoreType.DMA
    vmem = pl.BlockSpec(memory_space=pltpu.VMEM)
    gathered = pl.pallas_call(
        functools.partial(fused, n, inner, reach, tile),
        out_shape=jax.ShapeDtypeStruct((quarter, n * cols), bf16),
        in_specs=[vmem] * 3 + [pl.BlockSpec(memory_space=pl.ANY)],
        out_specs=vmem,
        scratch_shapes=[
            pltpu.VMEM((2, (reach + 1) * tok, HD), bf16),
            pltpu.VMEM((outer, 2, pieces, depth, cut), bf16),
            pltpu.VMEM((tok, depth), bf16),
            pltpu.VMEM((2, 2, 2 * block, depth), bf16),
            pltpu.VMEM((tok // tile, tile, reach * tok + tile), jnp.float32),
            pltpu.VMEM((2, outer, pieces, 2, block, cut), bf16),
            pltpu.VMEM((2, outer, pieces, block, cut), bf16),
            pltpu.VMEM((2, outer, pieces, inner, quarter, cut), bf16),
            dma((reach + 1, max(inner, reach + 1), 4)), dma((reach, 4)),
            dma((outer, 2, pieces)),
            dma((outer, pieces)), dma((outer, pieces)), dma((outer, pieces)),
            dma((inner, 2)), dma((inner, 2, 2)),
            dma((2,)), dma((inner, 2, 2)), dma((inner, 2, 2)),
            dma((2, outer, pieces)), dma((2, outer, pieces)),
            dma((2, outer, pieces, inner)), dma((outer, pieces, inner)),
        ],
        compiler_params=pltpu.CompilerParams(
            collective_id=0, has_side_effects=True, vmem_limit_bytes=60 * 1024 * 1024
        ),
    )(rot_q, pair, start, out_weight)
    return (gathered.astype(jnp.float32) + residual.astype(jnp.float32)).astype(jnp.bfloat16)


def solution(mesh):
    return jax.shard_map(
        on_device,
        mesh=mesh,
        in_specs=(
            P("ctx", "tp"),
            P("ctx", "tp"),
            P("ctx", "tp"),
            P(None, "ctx"),
            P(),
            P("tp", "ctx"),
            P(("ctx", "tp"), None),
        ),
        out_specs=P(("ctx", "tp"), None),
        check_vma=False,
    )
```

```python
import functools
import math

import jax
import jax.numpy as jnp
import numpy as np
from jax import lax
from jax.experimental import pallas as pl
from jax.experimental.pallas import tpu as pltpu
from jax.sharding import PartitionSpec as P

HD = 128
DOC = 2048

theta_base = 1000000.0
MESH_ID = pl.DeviceIdType.MESH


def half_frequencies():
    index = np.arange(HD // 2, dtype=np.float64)
    return np.power(theta_base, -2.0 * index / HD).astype(np.float32)[:, None]


def fused(
    n, inner, reach, tile,
    q_ref, k_ref, v_ref, place_ref, segment_ref, freq_ref, w_ref, out_ref,
    cosine, sine, my_segment, segments, kvbuf, wbuf, att, abuf, bias, pbuf, xrecv, obuf,
    kv_s, kv_r, w_r, wu_s, wd_s, wm_s, a_s, a_r, ha_s, hf_s, ha_r, x_s, x_r, o_s, o_r,
):
    outer = n // inner
    tok = q_ref.shape[0]
    pairs = q_ref.shape[1] // (2 * HD)
    tiles = tok // tile
    span = reach * tok + tile
    quarter = tok // 4
    pieces, cut = wbuf.shape[2], wbuf.shape[4]
    cols = w_ref.shape[1]
    block = inner * quarter
    chained = reach % inner == 0
    c = lax.axis_index("ctx")
    t = lax.axis_index("tp")
    co, ci = c // inner, c % inner
    x, h = t // 2, t % 2
    other_x = 1 - x
    last = outer - 1
    is_end = (co == 0) | (co == last)
    helps = (co == 1) | (co == last - 1)
    helped = jnp.where(co == 1, 0, last)
    helper = jnp.where(co == 0, 1, last - 1)
    mate = {"ctx": c, "tp": 2 * x + 1 - h}
    across = {"ctx": c, "tp": 2 * other_x + h}

    def remote(src, dst, send, recv, device):
        return pltpu.make_async_remote_copy(
            src_ref=src, dst_ref=dst, send_sem=send, recv_sem=recv,
            device_id=device, device_id_type=MESH_ID,
        )

    def landed(dst, sem):
        pltpu.make_async_copy(dst, dst, sem).wait()

    def own_piece(j):
        return pltpu.make_async_copy(
            w_ref.at[:, j * cut:(j + 1) * cut], wbuf.at[co, h, j], w_r.at[co, h, j]
        )

    for j in range(pieces):
        own_piece(j).start()

    barrier = pltpu.get_barrier_semaphore()

    def greet(device):
        pl.semaphore_signal(barrier, inc=1, device_id=device, device_id_type=MESH_ID)

    for k in range(inner):
        near = (ci + k) % inner
        for g in range(2):
            if k + g > 0:
                greet({"ctx": co * inner + near, "tp": 2 * x + (h + g) % 2})

            @pl.when(co < last)
            def _():
                greet({"ctx": (co + 1) * inner + near, "tp": 2 * x + g})

            @pl.when(co > 0)
            def _():
                greet({"ctx": (co - 1) * inner + near, "tp": 2 * x + g})
    greet(across)
    beside = jnp.where(co < last, 1, 0) + jnp.where(co > 0, 1, 0)

    def turned(vectors, at):
        wide = vectors.astype(jnp.float32)
        return (wide * cosine[at, :] + pltpu.roll(wide, HD // 2, 1) * sine[at, :]).astype(jnp.bfloat16)

    everything = pl.ds(0, tok)
    frequency = lax.broadcasted_iota(jnp.int32, (HD // 2, tok), 0)
    place = place_ref[...].astype(jnp.float32)
    first_end = HD // 8
    second_end = first_end + 3 * HD // 16
    chosen = jnp.where(
        frequency < first_end, place[0:1], jnp.where(frequency < second_end, place[1:2], place[2:3])
    )
    angle = chosen * freq_ref[...]
    cos_part, sin_part = jnp.cos(angle), jnp.sin(angle)
    cosine[...] = jnp.concatenate([cos_part, cos_part], axis=0).T
    sine[...] = jnp.concatenate([-sin_part, sin_part], axis=0).T
    kvbuf[0, reach * tok:, :] = turned(k_ref[...], everything)
    kvbuf[1, reach * tok:, :] = v_ref[...]
    pl.semaphore_wait(barrier, 2 * inner + 2 * inner * beside)

    half = tok // 2
    kv_parts = 4

    def kv_slot(d, part):
        start = pl.multiple_of((reach - d) * tok + part % 2 * half, half)
        return kvbuf.at[part // 2, pl.ds(start, half), :]

    def kv_sends(s, part, action):
        src = kv_slot(s * inner, part)
        if s == 0 and part // 2 == 1:
            src = v_ref.at[pl.ds(part % 2 * half, half), :]

        def one(k, slot, device):
            action(remote(src, kv_slot(slot, part), kv_s.at[s, k, part], kv_r.at[slot - 1, part], device))

        if not chained:
            for d in range(1, reach + 1):
                @pl.when(c + d < n)
                def _():
                    one(d, d, {"ctx": c + d, "tp": t})
            return

        @pl.when(co >= s)
        def _():
            if (s + 1) * inner <= reach:
                @pl.when(co < last)
                def _():
                    one(0, (s + 1) * inner, {"ctx": c + inner, "tp": t})
            for k in range(1, inner):
                near = (ci + k) % inner
                away = s * inner + near - ci

                @pl.when((away >= 1) & (away <= reach))
                def _():
                    one(k, away, {"ctx": co * inner + near, "tp": t})

    stages = reach // inner + 1 if chained else 1
    for part in range(kv_parts):
        kv_sends(0, part, lambda copy: copy.start())

    early = (pieces + 1) // 2
    shared = pieces // 2

    def w_up(slot, j):
        device = {"ctx": c + inner, "tp": t}
        return remote(wbuf.at[slot, h, j], wbuf.at[slot, h, j], wu_s.at[slot, j], w_r.at[slot, h, j], device)

    def w_down(slot, j):
        device = {"ctx": c - inner, "tp": t}
        return remote(wbuf.at[slot, h, j], wbuf.at[slot, h, j], wd_s.at[slot, j], w_r.at[slot, h, j], device)

    def w_mate(slot, j):
        return remote(wbuf.at[slot, h, j], wbuf.at[slot, h, j], wm_s.at[slot, j], w_r.at[slot, h, j], mate)

    def near_end(away, j):
        return (away <= 1) | ((away == 2) & (j < shared))

    def goes_up(slot, j):
        return (slot <= co) & (co < last) & ((co + 1 < last) | near_end(co + 1 - slot, j))

    def goes_down(slot, j):
        return (slot >= co) & (co > 0) & ((co > 1) | near_end(slot - co + 1, j))

    def has(slot, j):
        return jnp.logical_not(is_end) | (near_end(slot - co, j) & near_end(co - slot, j))

    def lends(slot, j):
        away = jnp.where(slot < helped, helped - slot, slot - helped)
        return helps & jnp.logical_not(near_end(away, j))

    def pass_up(slot, j):
        @pl.when(goes_up(slot, j))
        def _():
            w_up(slot, j).start()

    def pass_down(slot, j):
        @pl.when(goes_down(slot, j))
        def _():
            w_down(slot, j).start()

    def own_up():
        for j in range(pieces):
            if j < early:
                pass_up(co, j)
            else:
                @pl.when(jnp.logical_not(is_end))
                def _():
                    pass_up(co, j)

    for j in range(pieces):
        own_piece(j).wait()
        if j < early:
            pass_down(co, j)
        else:
            @pl.when(jnp.logical_not(is_end))
            def _():
                pass_down(co, j)
        w_mate(co, j).start()

    @pl.when(co == 0)
    def _():
        own_up()

    for d in range(reach + 1):
        @pl.when(c < d)
        def _():
            kvbuf[:, (reach - d) * tok:(reach - d + 1) * tok, :] = jnp.zeros((2, tok, HD), kvbuf.dtype)
            segments[:, (reach - d) * tok:(reach - d + 1) * tok] = jnp.full((1, tok), -1, jnp.int32)

        @pl.when(c >= d)
        def _():
            from_at = pl.multiple_of((c - d) * tok, tok)
            segments[:, (reach - d) * tok:(reach - d + 1) * tok] = segment_ref[:, pl.ds(from_at, tok)]
    own_ids = segments[:, reach * tok:].astype(jnp.float32)
    my_segment[...] = jnp.broadcast_to(own_ids, (HD, tok)).T

    def fill_bias(rt, _):
        at = pl.ds(pl.multiple_of(rt * tile, tile), tile)
        window = pl.ds(pl.multiple_of(rt * tile, tile), span)
        same = my_segment[at, 0:1] == segments[:, window].astype(jnp.float32)
        key = lax.broadcasted_iota(jnp.int32, (tile, span), 1)
        query = lax.broadcasted_iota(jnp.int32, (tile, span), 0) + reach * tok
        bias[rt] = jnp.where((key <= query) & same, 0.0, -1e30).astype(jnp.float32)
        return 0

    lax.fori_loop(0, tiles, fill_bias, 0)

    for s in range(1, stages):
        for part in range(kv_parts):
            @pl.when(co >= s)
            def _():
                landed(kv_slot(s * inner, part), kv_r.at[s * inner - 1, part])

            kv_sends(s, part, lambda copy: copy.start())
        if s == 1:
            @pl.when(co > 0)
            def _():
                own_up()

    if stages == 1:
        @pl.when(co > 0)
        def _():
            own_up()

    for d in range(1, reach + 1):
        if not chained or d % inner != 0:
            @pl.when(c >= d)
            def _():
                for part in range(kv_parts):
                    landed(kv_slot(d, part), kv_r.at[d - 1, part])

    factor = math.log2(math.e) / math.sqrt(HD)

    def rows_of(side, at):
        return pl.ds(pl.multiple_of((side * inner + at) * quarter, quarter), quarter)

    def a_copies(hp, action):
        lanes = pl.ds(pl.multiple_of(hp * 2 * HD, 2 * HD), 2 * HD)
        for side in range(2):
            for k in range(inner):
                near = (ci + k) % inner
                for gg in range(2):
                    g = (h + gg) % 2
                    src = att.at[pl.ds(pl.multiple_of((2 * side + g) * quarter, quarter), quarter), lanes]
                    if k + gg > 0:
                        action(remote(
                            src, abuf.at[0, h, rows_of(side, ci), lanes], a_s.at[k, gg],
                            a_r.at[ci, h, side], {"ctx": co * inner + near, "tp": 2 * x + g},
                        ))

                    if k == 0:
                        @pl.when(is_end)
                        def _():
                            action(remote(
                                src, abuf.at[1, h, rows_of(side, ci), lanes], ha_s.at[gg],
                                ha_r.at[ci, h, side], {"ctx": helper * inner + ci, "tp": 2 * x + g},
                            ))

    def attend(hp, _):
        lanes = pl.ds(pl.multiple_of(hp * 2 * HD, 2 * HD), 2 * HD)

        def one_tile(rt, _):
            at = pl.ds(pl.multiple_of(rt * tile, tile), tile)
            window = pl.ds(pl.multiple_of(rt * tile, tile), span)
            k = kvbuf[0, window, :]
            v = kvbuf[1, window, :]
            q2 = q_ref[at, lanes]
            done = []
            for e in range(2):
                q = turned(q2[:, e * HD:(e + 1) * HD], at)
                s = lax.dot_general(
                    q, k, (((1,), (1,)), ((), ())), preferred_element_type=jnp.float32
                ) + bias[rt]
                peak = jnp.max(s, axis=-1, keepdims=True)
                p = jnp.exp2((s - peak) * factor)
                total = jnp.sum(p, axis=-1, keepdims=True)
                mixed = jnp.dot(p.astype(jnp.bfloat16), v, preferred_element_type=jnp.float32)
                done.append((mixed / total).astype(jnp.bfloat16))
            att[at, lanes] = jnp.concatenate(done, axis=1)
            return 0

        lax.fori_loop(0, tiles, one_tile, 0)
        a_copies(hp, lambda copy: copy.start())
        for side in range(2):
            src = pl.ds(pl.multiple_of((2 * side + h) * quarter, quarter), quarter)
            abuf[0, h, rows_of(side, ci), lanes] = att[src, lanes]
        return 0

    lax.fori_loop(0, pairs, attend, 0)

    def each_side(distance, j, action):
        def one_side(side, _):
            slot = co + distance * (2 * side - 1)

            @pl.when((slot >= 0) & (slot < outer) & ((distance > 0) | (side == 1)))
            def _():
                @pl.when(has(slot, j))
                def _():
                    action(slot)
            return 0

        lax.fori_loop(0, 2, one_side, 0)

    def arrive(slot, j):
        landed(wbuf.at[slot, h, j], w_r.at[slot, h, j])
        pass_up(slot, j)
        pass_down(slot, j)
        w_mate(slot, j).start()

    def whole(slot, j):
        landed(wbuf.at[slot, 1 - h, j], w_r.at[slot, 1 - h, j])

    @pl.when(is_end)
    def _():
        for j in range(early, pieces):
            pass_up(co, j)
            pass_down(co, j)

    for j in range(early):
        each_side(1, j, lambda slot: arrive(slot, j))

    for k in range(inner):
        near = (ci + k) % inner
        for gg in range(2):
            if k + gg > 0:
                g = (h + gg) % 2
                for side in range(2):
                    landed(abuf.at[0, g, rows_of(side, near), :], a_r.at[near, g, side])

    def x_copy(who, slot, j):
        return remote(
            pbuf.at[who, slot, j, other_x], xrecv.at[who, slot, j],
            x_s.at[who, slot, j], x_r.at[who, slot, j], across,
        )

    def out_slot(slot, j, at):
        return out_ref.at[:, pl.ds(pl.multiple_of((slot * inner + at) * cols + j * cut, 128), cut)]

    def o_copy(who, slot, j, k):
        near = (ci + k) % inner
        node = helped if who else co
        device = {"ctx": node * inner + near, "tp": t}
        return remote(
            obuf.at[who, slot, j, near], out_slot(slot, j, ci),
            o_s.at[who, slot, j, k], o_r.at[slot, j, ci], device,
        )

    def job(who, slot, j):
        for side in range(2):
            at = slice(side * block, (side + 1) * block)
            pbuf[who, slot, j, side] = (
                jnp.dot(abuf[who, 0, at, :], wbuf[slot, 0, j], preferred_element_type=jnp.float32)
                + jnp.dot(abuf[who, 1, at, :], wbuf[slot, 1, j], preferred_element_type=jnp.float32)
            ).astype(jnp.bfloat16)
        x_copy(who, slot, j).start()

    def finish(who, slot, j):
        landed(xrecv.at[who, slot, j], x_r.at[who, slot, j])
        both = (
            pbuf[who, slot, j, x].astype(jnp.float32) + xrecv[who, slot, j].astype(jnp.float32)
        ).astype(jnp.bfloat16)
        for k in range(inner):
            obuf[who, slot, j, k] = both[k * quarter:(k + 1) * quarter]
        for k in range(1 - who, inner):
            o_copy(who, slot, j, k).start()
        if not who:
            out_ref[:, pl.ds(pl.multiple_of((slot * inner + ci) * cols + j * cut, 128), cut)] = obuf[who, slot, j, ci]

    beyond = 2 * co - helped

    def forwards(action):
        for k in range(1, inner):
            near = (ci + k) % inner
            for g in range(2):
                for side in range(2):
                    here = abuf.at[1, g, rows_of(side, ci), :]
                    action(remote(
                        here, here, hf_s.at[k, g, side], ha_r.at[ci, g, side],
                        {"ctx": co * inner + near, "tp": t},
                    ))

    def step(i, _):
        d, j = i // pieces, i % pieces

        @pl.when((d > 1) & (d < outer))
        def _():
            each_side(d, j, lambda slot: arrive(slot, j))

        @pl.when(helps & (i == 1))
        def _():
            for g in range(2):
                for side in range(2):
                    landed(abuf.at[1, g, rows_of(side, ci), :], ha_r.at[ci, g, side])
            forwards(lambda copy: copy.start())

        @pl.when(helps & (i == 2 * pieces))
        def _():
            for k in range(1, inner):
                near = (ci + k) % inner
                for g in range(2):
                    for side in range(2):
                        landed(abuf.at[1, g, rows_of(side, near), :], ha_r.at[near, g, side])

            def lend(jj, _):
                job(1, beyond, jj)
                return 0

            lax.fori_loop(shared, pieces, lend, 0)

        def begins(slot):
            whole(slot, j)

            @pl.when(lends(slot, j) & (d > 1))
            def _():
                job(1, slot, j)

            job(0, slot, j)

        @pl.when(d < outer)
        def _():
            each_side(d, j, begins)

        before = i - lag
        then = before % pieces

        @pl.when(before >= 0)
        def _():
            def ends(slot):
                @pl.when(lends(slot, then) & (before >= 2 * pieces))
                def _():
                    finish(1, slot, then)

                finish(0, slot, then)

            each_side(before // pieces, then, ends)

        @pl.when(helps & (d == 2) & (j >= shared))
        def _():
            finish(1, beyond, j)

        @pl.when((d == 1) & (j + early < pieces))
        def _():
            each_side(1, j, lambda slot: arrive(slot, j + early))
        return 0

    lag = min(5, pieces + 2)
    lax.fori_loop(0, outer * pieces + lag, step, 0)

    for s in range(stages):
        for part in range(kv_parts):
            kv_sends(s, part, lambda copy: copy.wait_send())
    for k in range(inner):
        for gg in range(2):
            if k + gg > 0:
                landed(abuf.at[0, 0, 0:2 * quarter, :], a_s.at[k, gg])

    @pl.when(is_end)
    def _():
        for gg in range(2):
            landed(abuf.at[0, 0, 0:2 * quarter, :], ha_s.at[gg])

    @pl.when(helps)
    def _():
        forwards(lambda copy: copy.wait_send())

    def drain(i, _):
        slot, j = i // pieces, i % pieces

        @pl.when(has(slot, j))
        def _():
            w_mate(slot, j).wait_send()

            @pl.when(goes_up(slot, j))
            def _():
                w_up(slot, j).wait_send()

            @pl.when(goes_down(slot, j))
            def _():
                w_down(slot, j).wait_send()

            x_copy(0, slot, j).wait_send()
            for k in range(1, inner):
                o_copy(0, slot, j, k).wait_send()

        @pl.when(lends(slot, j))
        def _():
            x_copy(1, slot, j).wait_send()
            for k in range(inner):
                o_copy(1, slot, j, k).wait_send()

        for k in range(inner):
            near = (ci + k) % inner
            if k == 0:
                @pl.when(jnp.logical_not(has(slot, j)))
                def _():
                    landed(out_slot(slot, j, near), o_r.at[slot, j, near])
            else:
                landed(out_slot(slot, j, near), o_r.at[slot, j, near])
        return 0

    lax.fori_loop(0, outer * pieces, drain, 0)


def on_device(queries, keys, values, positions, segment_ids, out_weight, residual):
    tok = queries.shape[0]
    n = lax.axis_size("ctx")
    inner = 2 ** max(1, int(math.log2(n)) // 2)
    outer = n // inner
    reach = (DOC + tok - 2) // tok
    tile = math.gcd(tok, 256)
    depth, cols = out_weight.shape
    cut = math.gcd(cols, 128)
    pieces = cols // cut
    quarter = tok // 4
    block = inner * quarter
    bf16 = jnp.bfloat16
    dma = pltpu.SemaphoreType.DMA
    vmem = pl.BlockSpec(memory_space=pltpu.VMEM)
    gathered = pl.pallas_call(
        functools.partial(fused, n, inner, reach, tile),
        out_shape=jax.ShapeDtypeStruct((quarter, n * cols), bf16),
        in_specs=[vmem] * 6 + [pl.BlockSpec(memory_space=pl.ANY)],
        out_specs=vmem,
        scratch_shapes=[
            pltpu.VMEM((tok, HD), jnp.float32),
            pltpu.VMEM((tok, HD), jnp.float32),
            pltpu.VMEM((tok, HD), jnp.float32),
            pltpu.VMEM((1, (reach + 1) * tok), jnp.int32),
            pltpu.VMEM((2, (reach + 1) * tok, HD), bf16),
            pltpu.VMEM((outer, 2, pieces, depth, cut), bf16),
            pltpu.VMEM((tok, depth), bf16),
            pltpu.VMEM((2, 2, 2 * block, depth), bf16),
            pltpu.VMEM((tok // tile, tile, reach * tok + tile), jnp.float32),
            pltpu.VMEM((2, outer, pieces, 2, block, cut), bf16),
            pltpu.VMEM((2, outer, pieces, block, cut), bf16),
            pltpu.VMEM((2, outer, pieces, inner, quarter, cut), bf16),
            dma((reach + 1, max(inner, reach + 1), 4)), dma((reach, 4)),
            dma((outer, 2, pieces)),
            dma((outer, pieces)), dma((outer, pieces)), dma((outer, pieces)),
            dma((inner, 2)), dma((inner, 2, 2)),
            dma((2,)), dma((inner, 2, 2)), dma((inner, 2, 2)),
            dma((2, outer, pieces)), dma((2, outer, pieces)),
            dma((2, outer, pieces, inner)), dma((outer, pieces, inner)),
        ],
        compiler_params=pltpu.CompilerParams(
            collective_id=0, has_side_effects=True, vmem_limit_bytes=60 * 1024 * 1024
        ),
    )(queries, keys, values, positions, segment_ids[None, :], half_frequencies(), out_weight)
    return (gathered.astype(jnp.float32) + residual.astype(jnp.float32)).astype(jnp.bfloat16)


def solution(mesh):
    return jax.shard_map(
        on_device,
        mesh=mesh,
        in_specs=(
            P("ctx", "tp"),
            P("ctx", "tp"),
            P("ctx", "tp"),
            P(None, "ctx"),
            P(),
            P("tp", "ctx"),
            P(("ctx", "tp"), None),
        ),
        out_specs=P(("ctx", "tp"), None),
        check_vma=False,
    )
```

```python
import functools
import math

import jax
import jax.numpy as jnp
import numpy as np
from jax import lax
from jax.experimental import pallas as pl
from jax.experimental.pallas import tpu as pltpu
from jax.sharding import PartitionSpec as P

HD = 128
DOC = 2048

theta_base = 1000000.0
MESH_ID = pl.DeviceIdType.MESH


def half_frequencies():
    index = np.arange(HD // 2, dtype=np.float64)
    values = np.power(theta_base, -2.0 * index / HD).astype(np.float32)
    return np.broadcast_to(values[:, None], (HD // 2, HD)).copy()


def fused(
    n, inner, reach, tile,
    k_hbm, v_hbm, place_hbm, segment_hbm, freq_hbm, q_hbm, w_ref, out_ref,
    k_ref, v_ref, place_ref, segment_ref, freq_ref, q_ref, cosine, sine, my_segment, segments, kvbuf, wbuf, att, abuf, bias, pbuf, xrecv, obuf,
    in_s, kv_s, kv_r, w_r, wu_s, wd_s, wm_s, a_s, a_r, ha_s, hf_s, ha_r, x_s, x_r, o_s, o_r,
):
    outer = n // inner
    tok = q_ref.shape[0]
    pairs = q_ref.shape[1] // (2 * HD)
    tiles = tok // tile
    span = reach * tok + tile
    quarter = tok // 4
    pieces, cut = wbuf.shape[2], wbuf.shape[4]
    cols = w_ref.shape[1]
    block = inner * quarter
    chained = reach % inner == 0
    c = lax.axis_index("ctx")
    t = lax.axis_index("tp")
    co, ci = c // inner, c % inner
    x, h = t // 2, t % 2
    other_x = 1 - x
    last = outer - 1
    is_end = (co == 0) | (co == last)
    helps = (co == 1) | (co == last - 1)
    helped = jnp.where(co == 1, 0, last)
    helper = jnp.where(co == 0, 1, last - 1)
    mate = {"ctx": c, "tp": 2 * x + 1 - h}
    across = {"ctx": c, "tp": 2 * other_x + h}

    def remote(src, dst, send, recv, device):
        return pltpu.make_async_remote_copy(
            src_ref=src, dst_ref=dst, send_sem=send, recv_sem=recv,
            device_id=device, device_id_type=MESH_ID,
        )

    def landed(dst, sem):
        pltpu.make_async_copy(dst, dst, sem).wait()

    def own_piece(j):
        return pltpu.make_async_copy(
            w_ref.at[:, j * cut:(j + 1) * cut], wbuf.at[co, h, j], w_r.at[co, h, j]
        )

    moves = [
        pltpu.make_async_copy(src, dst, in_s.at[k]) for k, (src, dst) in enumerate([
            (place_hbm, place_ref), (freq_hbm, freq_ref), (k_hbm, k_ref), (v_hbm, v_ref),
            (segment_hbm, segment_ref), (q_hbm, q_ref),
        ])
    ]
    q_copy = moves[-1]
    for move in moves:
        move.start()
    for j in range(pieces):
        own_piece(j).start()

    barrier = pltpu.get_barrier_semaphore()

    def greet(device):
        pl.semaphore_signal(barrier, inc=1, device_id=device, device_id_type=MESH_ID)

    for k in range(inner):
        near = (ci + k) % inner
        for g in range(2):
            if k + g > 0:
                greet({"ctx": co * inner + near, "tp": 2 * x + (h + g) % 2})

            @pl.when(co < last)
            def _():
                greet({"ctx": (co + 1) * inner + near, "tp": 2 * x + g})

            @pl.when(co > 0)
            def _():
                greet({"ctx": (co - 1) * inner + near, "tp": 2 * x + g})
    greet(across)
    beside = jnp.where(co < last, 1, 0) + jnp.where(co > 0, 1, 0)

    def turned(vectors, at):
        wide = vectors.astype(jnp.float32)
        return (wide * cosine[at, :] + pltpu.roll(wide, HD // 2, 1) * sine[at, :]).astype(jnp.bfloat16)

    pl.semaphore_wait(barrier, 2 * inner + 2 * inner * beside)
    for move in moves[:-1]:
        move.wait()

    half = tok // 2
    kv_parts = 4

    def kv_slot(d, part):
        start = pl.multiple_of((reach - d) * tok + part % 2 * half, half)
        return kvbuf.at[part // 2, pl.ds(start, half), :]

    def kv_sends(s, part, action):
        src = kv_slot(s * inner, part)
        if s == 0 and part // 2 == 1:
            src = v_ref.at[pl.ds(part % 2 * half, half), :]

        def one(k, slot, device):
            action(remote(src, kv_slot(slot, part), kv_s.at[s, k], kv_r.at[slot - 1, part], device))

        if not chained:
            for d in range(1, reach + 1):
                @pl.when(c + d < n)
                def _():
                    one(d, d, {"ctx": c + d, "tp": t})
            return

        @pl.when(co >= s)
        def _():
            if (s + 1) * inner <= reach:
                @pl.when(co < last)
                def _():
                    one(0, (s + 1) * inner, {"ctx": c + inner, "tp": t})
            for k in range(1, inner):
                near = (ci + k) % inner
                away = s * inner + near - ci

                @pl.when((away >= 1) & (away <= reach))
                def _():
                    one(k, away, {"ctx": co * inner + near, "tp": t})

    stages = reach // inner + 1 if chained else 1
    for part in range(2, kv_parts):
        kv_sends(0, part, lambda copy: copy.start())

    early = (pieces + 1) // 2
    shared = pieces * 5 // 8

    def w_up(slot, j):
        device = {"ctx": c + inner, "tp": t}
        return remote(wbuf.at[slot, h, j], wbuf.at[slot, h, j], wu_s.at[slot], w_r.at[slot, h, j], device)

    def w_down(slot, j):
        device = {"ctx": c - inner, "tp": t}
        return remote(wbuf.at[slot, h, j], wbuf.at[slot, h, j], wd_s.at[slot], w_r.at[slot, h, j], device)

    def w_mate(slot, j):
        return remote(wbuf.at[slot, h, j], wbuf.at[slot, h, j], wm_s.at[slot], w_r.at[slot, h, j], mate)

    def near_end(away, j):
        return (away <= 1) | ((away == 2) & (j < shared))

    def goes_up(slot, j):
        return (slot <= co) & (co < last) & ((co + 1 < last) | near_end(co + 1 - slot, j))

    def goes_down(slot, j):
        return (slot >= co) & (co > 0) & ((co > 1) | near_end(slot - co + 1, j))

    def has(slot, j):
        return jnp.logical_not(is_end) | (near_end(slot - co, j) & near_end(co - slot, j))

    def lends(slot, j):
        away = jnp.where(slot < helped, helped - slot, slot - helped)
        return helps & jnp.logical_not(near_end(away, j))

    def pass_up(slot, j):
        @pl.when(goes_up(slot, j))
        def _():
            w_up(slot, j).start()

    def pass_down(slot, j):
        @pl.when(goes_down(slot, j))
        def _():
            w_down(slot, j).start()

    def own_up():
        for j in range(pieces):
            if j < early:
                pass_up(co, j)
            else:
                @pl.when(jnp.logical_not(is_end))
                def _():
                    pass_up(co, j)

    for j in range(pieces):
        own_piece(j).wait()
        if j < early:
            pass_down(co, j)
        else:
            @pl.when(jnp.logical_not(is_end))
            def _():
                pass_down(co, j)
        w_mate(co, j).start()

    everything = pl.ds(0, tok)
    frequency = lax.broadcasted_iota(jnp.int32, (HD // 2, tok), 0)
    place = place_ref[...].astype(jnp.float32)
    first_end = HD // 8
    second_end = first_end + 3 * HD // 16
    chosen = jnp.where(
        frequency < first_end, place[0:1], jnp.where(frequency < second_end, place[1:2], place[2:3])
    )
    angle = chosen * freq_ref[:, 0:1]
    cos_part, sin_part = jnp.cos(angle), jnp.sin(angle)
    cosine[...] = jnp.concatenate([cos_part, cos_part], axis=0).T
    sine[...] = jnp.concatenate([-sin_part, sin_part], axis=0).T
    kvbuf[0, reach * tok:, :] = turned(k_ref[...], everything)
    kvbuf[1, reach * tok:, :] = v_ref[...]
    for part in range(2):
        kv_sends(0, part, lambda copy: copy.start())

    @pl.when(co == 0)
    def _():
        own_up()

    for d in range(reach + 1):
        @pl.when(c < d)
        def _():
            kvbuf[:, (reach - d) * tok:(reach - d + 1) * tok, :] = jnp.zeros((2, tok, HD), kvbuf.dtype)
            segments[:, (reach - d) * tok:(reach - d + 1) * tok] = jnp.full((1, tok), -1, jnp.int32)

        @pl.when(c >= d)
        def _():
            from_at = pl.multiple_of((c - d) * tok, tok)
            segments[:, (reach - d) * tok:(reach - d + 1) * tok] = segment_ref[:, pl.ds(from_at, tok)]
    own_ids = segments[:, reach * tok:].astype(jnp.float32)
    my_segment[...] = jnp.broadcast_to(own_ids, (HD, tok)).T

    def fill_bias(rt, _):
        at = pl.ds(pl.multiple_of(rt * tile, tile), tile)
        window = pl.ds(pl.multiple_of(rt * tile, tile), span)
        same = my_segment[at, 0:1] == segments[:, window].astype(jnp.float32)
        key = lax.broadcasted_iota(jnp.int32, (tile, span), 1)
        query = lax.broadcasted_iota(jnp.int32, (tile, span), 0) + reach * tok
        bias[rt] = jnp.where((key <= query) & same, 0.0, -1e30).astype(jnp.float32)
        return 0

    lax.fori_loop(0, tiles, fill_bias, 0)

    for s in range(1, stages):
        for part in (2, 3, 0, 1):
            @pl.when(co >= s)
            def _():
                landed(kv_slot(s * inner, part), kv_r.at[s * inner - 1, part])

            kv_sends(s, part, lambda copy: copy.start())
        if s == 1:
            @pl.when(co > 0)
            def _():
                own_up()

    if stages == 1:
        @pl.when(co > 0)
        def _():
            own_up()

    for d in range(1, reach + 1):
        if not chained or d % inner != 0:
            @pl.when(c >= d)
            def _():
                for part in range(kv_parts):
                    landed(kv_slot(d, part), kv_r.at[d - 1, part])

    q_copy.wait()
    factor = math.log2(math.e) / math.sqrt(HD)

    def rows_of(side, at):
        return pl.ds(pl.multiple_of((side * inner + at) * quarter, quarter), quarter)

    def a_copies(hp, action):
        lanes = pl.ds(pl.multiple_of(hp * 2 * HD, 2 * HD), 2 * HD)
        for side in range(2):
            for k in range(inner):
                near = (ci + k) % inner
                for gg in range(2):
                    g = (h + gg) % 2
                    src = att.at[pl.ds(pl.multiple_of((2 * side + g) * quarter, quarter), quarter), lanes]
                    if k + gg > 0:
                        action(remote(
                            src, abuf.at[0, h, rows_of(side, ci), lanes], a_s.at[k, gg],
                            a_r.at[ci, h, side], {"ctx": co * inner + near, "tp": 2 * x + g},
                        ))

                    if k == 0:
                        @pl.when(is_end)
                        def _():
                            action(remote(
                                src, abuf.at[1, h, rows_of(side, ci), lanes], ha_s,
                                ha_r.at[ci, h, side], {"ctx": helper * inner + ci, "tp": 2 * x + g},
                            ))

    def attend(hp, _):
        lanes = pl.ds(pl.multiple_of(hp * 2 * HD, 2 * HD), 2 * HD)

        def one_tile(rt, _):
            at = pl.ds(pl.multiple_of(rt * tile, tile), tile)
            window = pl.ds(pl.multiple_of(rt * tile, tile), span)
            k = kvbuf[0, window, :]
            v = kvbuf[1, window, :]
            q2 = q_ref[at, lanes]
            done = []
            for e in range(2):
                q = turned(q2[:, e * HD:(e + 1) * HD], at)
                s = lax.dot_general(
                    q, k, (((1,), (1,)), ((), ())), preferred_element_type=jnp.float32
                ) + bias[rt]
                peak = jnp.max(s, axis=-1, keepdims=True)
                p = jnp.exp2((s - peak) * factor)
                total = jnp.sum(p, axis=-1, keepdims=True)
                mixed = jnp.dot(p.astype(jnp.bfloat16), v, preferred_element_type=jnp.float32)
                done.append((mixed / total).astype(jnp.bfloat16))
            att[at, lanes] = jnp.concatenate(done, axis=1)
            return 0

        lax.fori_loop(0, tiles, one_tile, 0)
        a_copies(hp, lambda copy: copy.start())
        for side in range(2):
            src = pl.ds(pl.multiple_of((2 * side + h) * quarter, quarter), quarter)
            abuf[0, h, rows_of(side, ci), lanes] = att[src, lanes]
        return 0

    lax.fori_loop(0, pairs, attend, 0)

    def each_side(distance, j, action):
        def one_side(side, _):
            slot = co + distance * (2 * side - 1)

            @pl.when((slot >= 0) & (slot < outer) & ((distance > 0) | (side == 1)))
            def _():
                @pl.when(has(slot, j))
                def _():
                    action(slot)
            return 0

        lax.fori_loop(0, 2, one_side, 0)

    def arrive(slot, j):
        landed(wbuf.at[slot, h, j], w_r.at[slot, h, j])
        pass_up(slot, j)
        pass_down(slot, j)
        w_mate(slot, j).start()

    def whole(slot, j):
        landed(wbuf.at[slot, 1 - h, j], w_r.at[slot, 1 - h, j])

    @pl.when(is_end)
    def _():
        for j in range(early, pieces):
            pass_up(co, j)
            pass_down(co, j)

    for j in range(early):
        each_side(1, j, lambda slot: arrive(slot, j))

    for k in range(inner):
        near = (ci + k) % inner
        for gg in range(2):
            if k + gg > 0:
                g = (h + gg) % 2
                for side in range(2):
                    landed(abuf.at[0, g, rows_of(side, near), :], a_r.at[near, g, side])

    def x_copy(who, slot, j):
        return remote(
            pbuf.at[who, slot, j, other_x], xrecv.at[who, slot, j],
            x_s.at[who, slot], x_r.at[who, slot, j], across,
        )

    def out_slot(slot, j, at):
        return out_ref.at[:, pl.ds(pl.multiple_of((slot * inner + at) * cols + j * cut, 128), cut)]

    def o_copy(who, slot, j, k):
        near = (ci + k) % inner
        node = helped if who else co
        device = {"ctx": node * inner + near, "tp": t}
        return remote(
            obuf.at[who, slot, j, near], out_slot(slot, j, ci),
            o_s.at[who, slot], o_r.at[slot, ci], device,
        )

    def job(who, slot, j):
        for side in range(2):
            at = slice(side * block, (side + 1) * block)
            pbuf[who, slot, j, side] = (
                jnp.dot(abuf[who, 0, at, :], wbuf[slot, 0, j], preferred_element_type=jnp.float32)
                + jnp.dot(abuf[who, 1, at, :], wbuf[slot, 1, j], preferred_element_type=jnp.float32)
            ).astype(jnp.bfloat16)
        x_copy(who, slot, j).start()

    def finish(who, slot, j):
        landed(xrecv.at[who, slot, j], x_r.at[who, slot, j])
        both = (
            pbuf[who, slot, j, x].astype(jnp.float32) + xrecv[who, slot, j].astype(jnp.float32)
        ).astype(jnp.bfloat16)
        for k in range(inner):
            obuf[who, slot, j, k] = both[k * quarter:(k + 1) * quarter]
        for k in range(1 - who, inner):
            o_copy(who, slot, j, k).start()
        if not who:
            out_ref[:, pl.ds(pl.multiple_of((slot * inner + ci) * cols + j * cut, 128), cut)] = obuf[who, slot, j, ci]

    beyond = 2 * co - helped

    def forwards(action):
        for k in range(1, inner):
            near = (ci + k) % inner
            for g in range(2):
                for side in range(2):
                    here = abuf.at[1, g, rows_of(side, ci), :]
                    action(remote(
                        here, here, hf_s, ha_r.at[ci, g, side],
                        {"ctx": co * inner + near, "tp": t},
                    ))

    lag = min(5, pieces + 2)
    ahead = min(2, early)
    forward_at = max(1, min(5, pieces - 1))

    def step(i, _):
        d, j = i // pieces, i % pieces

        @pl.when((d > 1) & (d < outer))
        def _():
            each_side(d, j, lambda slot: arrive(slot, j))

        @pl.when(helps & (i == forward_at))
        def _():
            for g in range(2):
                for side in range(2):
                    landed(abuf.at[1, g, rows_of(side, ci), :], ha_r.at[ci, g, side])
            forwards(lambda copy: copy.start())

        @pl.when(helps & (i == 2 * pieces))
        def _():
            for k in range(1, inner):
                near = (ci + k) % inner
                for g in range(2):
                    for side in range(2):
                        landed(abuf.at[1, g, rows_of(side, near), :], ha_r.at[near, g, side])

            def lend(jj, _):
                job(1, beyond, jj)
                return 0

            lax.fori_loop(shared, pieces, lend, 0)

        def begins(slot):
            whole(slot, j)

            @pl.when(lends(slot, j) & (d > 1))
            def _():
                job(1, slot, j)

            job(0, slot, j)

        @pl.when(d < outer)
        def _():
            each_side(d, j, begins)

        before = i - lag
        then = before % pieces

        @pl.when(before >= 0)
        def _():
            def ends(slot):
                @pl.when(lends(slot, then) & (before >= 2 * pieces))
                def _():
                    finish(1, slot, then)

                finish(0, slot, then)

            each_side(before // pieces, then, ends)

        @pl.when(helps & (d == 2) & (j >= shared))
        def _():
            finish(1, beyond, j)

        @pl.when((d == 1) & (j + ahead >= early) & (j + ahead < pieces))
        def _():
            each_side(1, j, lambda slot: arrive(slot, j + ahead))
        return 0

    lax.fori_loop(0, outer * pieces + lag, step, 0)

    def kv_sent(s, k):
        landed(kvbuf.at[:, 0:tok, :], kv_s.at[s, k])

    if chained:
        for s in range(stages):
            @pl.when(co >= s)
            def _():
                if (s + 1) * inner <= reach:
                    @pl.when(co < last)
                    def _():
                        kv_sent(s, 0)
                for k in range(1, inner):
                    away = s * inner + (ci + k) % inner - ci

                    @pl.when((away >= 1) & (away <= reach))
                    def _():
                        kv_sent(s, k)
    else:
        for d in range(1, reach + 1):
            @pl.when(c + d < n)
            def _():
                kv_sent(0, d)
    for k in range(inner):
        for gg in range(2):
            if k + gg > 0:
                landed(abuf.at[0, 0, 0:2 * quarter, :], a_s.at[k, gg])

    @pl.when(is_end)
    def _():
        landed(abuf.at[0, :, 0:2 * quarter, :], ha_s)

    @pl.when(helps)
    def _():
        landed(abuf.at[1, :, 0:2 * quarter * (inner - 1), :], hf_s)

    def drain(slot, _):
        def parted(action):
            whole_unit = has(slot, pieces - 1)

            @pl.when(whole_unit)
            def _():
                action(pieces)

            if shared:
                @pl.when(has(slot, 0) & jnp.logical_not(whole_unit))
                def _():
                    action(shared)

        def sent(count):
            landed(wbuf.at[slot, h, 0:count], wm_s.at[slot])
            landed(xrecv.at[0, slot, 0:count], x_s.at[0, slot])
            landed(obuf.at[0, slot, 0:count, 0:inner - 1], o_s.at[0, slot])

        parted(sent)

        def moved(goes, sem):
            whole_unit = goes(slot, pieces - 1)

            @pl.when(whole_unit)
            def _():
                landed(wbuf.at[slot, h], sem)

            if shared:
                @pl.when(goes(slot, 0) & jnp.logical_not(whole_unit))
                def _():
                    landed(wbuf.at[slot, h, 0:shared], sem)

        moved(goes_up, wu_s.at[slot])
        moved(goes_down, wd_s.at[slot])

        def lent(start):
            landed(xrecv.at[1, slot, start:pieces], x_s.at[1, slot])
            landed(obuf.at[1, slot, start:pieces], o_s.at[1, slot])

        @pl.when(lends(slot, 0))
        def _():
            lent(0)

        if shared:
            @pl.when(lends(slot, pieces - 1) & jnp.logical_not(lends(slot, 0)))
            def _():
                lent(shared)

        def unit(at, start):
            first = pl.multiple_of((slot * inner + at) * cols + start * cut, 128)
            return out_ref.at[:, pl.ds(first, cols - start * cut)]

        @pl.when(jnp.logical_not(has(slot, 0)))
        def _():
            landed(unit(ci, 0), o_r.at[slot, ci])

        if shared:
            @pl.when(has(slot, 0) & jnp.logical_not(has(slot, pieces - 1)))
            def _():
                landed(unit(ci, shared), o_r.at[slot, ci])

        for k in range(1, inner):
            near = (ci + k) % inner
            landed(unit(near, 0), o_r.at[slot, near])
        return 0

    lax.fori_loop(0, outer, drain, 0)


def on_device(queries, keys, values, positions, segment_ids, out_weight, residual):
    tok = queries.shape[0]
    n = lax.axis_size("ctx")
    inner = 2 ** max(1, int(math.log2(n)) // 2)
    outer = n // inner
    reach = (DOC + tok - 2) // tok
    tile = math.gcd(tok, 256)
    depth, cols = out_weight.shape
    cut = math.gcd(cols, 128)
    pieces = cols // cut
    quarter = tok // 4
    block = inner * quarter
    bf16 = jnp.bfloat16
    dma = pltpu.SemaphoreType.DMA
    vmem = pl.BlockSpec(memory_space=pltpu.VMEM)
    gathered = pl.pallas_call(
        functools.partial(fused, n, inner, reach, tile),
        out_shape=jax.ShapeDtypeStruct((quarter, n * cols), bf16),
        in_specs=[pl.BlockSpec(memory_space=pltpu.HBM)] * 7,
        out_specs=vmem,
        scratch_shapes=[
            pltpu.VMEM((tok, HD), bf16),
            pltpu.VMEM((tok, HD), bf16),
            pltpu.VMEM(positions.shape, jnp.int32),
            pltpu.VMEM((1, n * tok), jnp.int32),
            pltpu.VMEM((HD // 2, HD), jnp.float32),
            pltpu.VMEM((tok, depth), bf16),
            pltpu.VMEM((tok, HD), jnp.float32),
            pltpu.VMEM((tok, HD), jnp.float32),
            pltpu.VMEM((tok, HD), jnp.float32),
            pltpu.VMEM((1, (reach + 1) * tok), jnp.int32),
            pltpu.VMEM((2, (reach + 1) * tok, HD), bf16),
            pltpu.VMEM((outer, 2, pieces, depth, cut), bf16),
            pltpu.VMEM((tok, depth), bf16),
            pltpu.VMEM((2, 2, 2 * block, depth), bf16),
            pltpu.VMEM((tok // tile, tile, reach * tok + tile), jnp.float32),
            pltpu.VMEM((2, outer, pieces, 2, block, cut), bf16),
            pltpu.VMEM((2, outer, pieces, block, cut), bf16),
            pltpu.VMEM((2, outer, pieces, inner, quarter, cut), bf16),
            dma((6,)),
            dma((reach // inner + 1, inner) if reach % inner == 0 else (1, reach + 1)), dma((reach, 4)),
            dma((outer, 2, pieces)), dma((outer,)), dma((outer,)), dma((outer,)),
            dma((inner, 2)), dma((inner, 2, 2)),
            dma, dma, dma((inner, 2, 2)),
            dma((2, outer)), dma((2, outer, pieces)),
            dma((2, outer)), dma((outer, inner)),
        ],
        compiler_params=pltpu.CompilerParams(
            collective_id=0, has_side_effects=True, vmem_limit_bytes=60 * 1024 * 1024
        ),
    )(keys, values, positions, segment_ids[None, :], half_frequencies(), queries, out_weight)
    return (gathered.astype(jnp.float32) + residual.astype(jnp.float32)).astype(jnp.bfloat16)


def solution(mesh):
    return jax.shard_map(
        on_device,
        mesh=mesh,
        in_specs=(
            P("ctx", "tp"),
            P("ctx", "tp"),
            P("ctx", "tp"),
            P(None, "ctx"),
            P(),
            P("tp", "ctx"),
            P(("ctx", "tp"), None),
        ),
        out_specs=P(("ctx", "tp"), None),
        check_vma=False,
    )
```

```python
import functools
import math

import jax
import jax.numpy as jnp
import numpy as np
from jax import lax
from jax.experimental import pallas as pl
from jax.experimental.pallas import tpu as pltpu
from jax.sharding import PartitionSpec as P

HD = 128
DOC = 2048

theta_base = 1000000.0
MESH_ID = pl.DeviceIdType.MESH


def half_frequencies():
    index = np.arange(HD // 2, dtype=np.float64)
    values = np.power(theta_base, -2.0 * index / HD).astype(np.float32)
    return np.broadcast_to(values[:, None], (HD // 2, HD)).copy()


def fused(
    n, inner, reach, tile,
    k_hbm, v_hbm, place_hbm, segment_hbm, freq_hbm, q_hbm, residual_hbm, w_ref, result_hbm,
    k_ref, v_ref, place_ref, segment_ref, freq_ref, q_ref, residual_ref, out_ref, cosine, sine, my_segment, segments, kvbuf, wbuf, att, abuf, bias, pbuf, xrecv, obuf,
    in_s, out_s, kv_s, kv_r, w_r, wu_s, wd_s, wm_s, a_s, a_r, ha_s, hf_s, ha_r, x_s, x_r, o_s, o_r,
):
    outer = n // inner
    tok = q_ref.shape[0]
    pairs = q_ref.shape[1] // (2 * HD)
    tiles = tok // tile
    span = reach * tok + tile
    quarter = tok // 4
    pieces, cut = wbuf.shape[2], wbuf.shape[4]
    cols = w_ref.shape[1]
    block = inner * quarter
    chained = reach % inner == 0
    c = lax.axis_index("ctx")
    t = lax.axis_index("tp")
    co, ci = c // inner, c % inner
    x, h = t // 2, t % 2
    other_x = 1 - x
    last = outer - 1
    is_end = (co == 0) | (co == last)
    helps = (co == 1) | (co == last - 1)
    helped = jnp.where(co == 1, 0, last)
    helper = jnp.where(co == 0, 1, last - 1)
    mate = {"ctx": c, "tp": 2 * x + 1 - h}
    across = {"ctx": c, "tp": 2 * other_x + h}

    def remote(src, dst, send, recv, device):
        return pltpu.make_async_remote_copy(
            src_ref=src, dst_ref=dst, send_sem=send, recv_sem=recv,
            device_id=device, device_id_type=MESH_ID,
        )

    def landed(dst, sem):
        pltpu.make_async_copy(dst, dst, sem).wait()

    def own_piece(j):
        return pltpu.make_async_copy(
            w_ref.at[:, j * cut:(j + 1) * cut], wbuf.at[co, h, j], w_r.at[co, h, j]
        )

    moves = [
        pltpu.make_async_copy(src, dst, in_s.at[k]) for k, (src, dst) in enumerate([
            (place_hbm, place_ref), (freq_hbm, freq_ref), (k_hbm, k_ref), (v_hbm, v_ref),
            (segment_hbm, segment_ref), (q_hbm, q_ref), (residual_hbm, residual_ref),
        ])
    ]
    q_copy, residual_copy = moves[-2:]
    for move in moves[:-1]:
        move.start()
    for j in range(pieces):
        own_piece(j).start()

    barrier = pltpu.get_barrier_semaphore()

    def greet(device):
        pl.semaphore_signal(barrier, inc=1, device_id=device, device_id_type=MESH_ID)

    for k in range(inner):
        near = (ci + k) % inner
        for g in range(2):
            if k + g > 0:
                greet({"ctx": co * inner + near, "tp": 2 * x + (h + g) % 2})

            @pl.when(co < last)
            def _():
                greet({"ctx": (co + 1) * inner + near, "tp": 2 * x + g})

            @pl.when(co > 0)
            def _():
                greet({"ctx": (co - 1) * inner + near, "tp": 2 * x + g})
    greet(across)
    beside = jnp.where(co < last, 1, 0) + jnp.where(co > 0, 1, 0)

    def turned(vectors, at):
        wide = vectors.astype(jnp.float32)
        return (wide * cosine[at, :] + pltpu.roll(wide, HD // 2, 1) * sine[at, :]).astype(jnp.bfloat16)

    pl.semaphore_wait(barrier, 2 * inner + 2 * inner * beside)
    residual_copy.start()
    for move in moves[:-2]:
        move.wait()

    half = tok // 2
    kv_parts = 4

    def kv_slot(d, part):
        start = pl.multiple_of((reach - d) * tok + part % 2 * half, half)
        return kvbuf.at[part // 2, pl.ds(start, half), :]

    def kv_sends(s, part, action):
        src = kv_slot(s * inner, part)
        if s == 0 and part // 2 == 1:
            src = v_ref.at[pl.ds(part % 2 * half, half), :]

        def one(k, slot, device):
            action(remote(src, kv_slot(slot, part), kv_s.at[s, k], kv_r.at[slot - 1, part], device))

        if not chained:
            for d in range(1, reach + 1):
                @pl.when(c + d < n)
                def _():
                    one(d, d, {"ctx": c + d, "tp": t})
            return

        @pl.when(co >= s)
        def _():
            if (s + 1) * inner <= reach:
                @pl.when(co < last)
                def _():
                    one(0, (s + 1) * inner, {"ctx": c + inner, "tp": t})
            for k in range(1, inner):
                near = (ci + k) % inner
                away = s * inner + near - ci

                @pl.when((away >= 1) & (away <= reach))
                def _():
                    one(k, away, {"ctx": co * inner + near, "tp": t})

    stages = reach // inner + 1 if chained else 1
    for part in range(2, kv_parts):
        kv_sends(0, part, lambda copy: copy.start())

    early = (pieces + 1) // 2
    shared = pieces * 5 // 8

    def w_up(slot, j):
        device = {"ctx": c + inner, "tp": t}
        return remote(wbuf.at[slot, h, j], wbuf.at[slot, h, j], wu_s.at[slot], w_r.at[slot, h, j], device)

    def w_down(slot, j):
        device = {"ctx": c - inner, "tp": t}
        return remote(wbuf.at[slot, h, j], wbuf.at[slot, h, j], wd_s.at[slot], w_r.at[slot, h, j], device)

    def w_mate(slot, j):
        return remote(wbuf.at[slot, h, j], wbuf.at[slot, h, j], wm_s.at[slot], w_r.at[slot, h, j], mate)

    def near_end(away, j):
        return (away <= 1) | ((away == 2) & (j < shared))

    def goes_up(slot, j):
        return (slot <= co) & (co < last) & ((co + 1 < last) | near_end(co + 1 - slot, j))

    def goes_down(slot, j):
        return (slot >= co) & (co > 0) & ((co > 1) | near_end(slot - co + 1, j))

    def has(slot, j):
        return jnp.logical_not(is_end) | (near_end(slot - co, j) & near_end(co - slot, j))

    def lends(slot, j):
        away = jnp.where(slot < helped, helped - slot, slot - helped)
        return helps & jnp.logical_not(near_end(away, j))

    def pass_up(slot, j):
        @pl.when(goes_up(slot, j))
        def _():
            w_up(slot, j).start()

    def pass_down(slot, j):
        @pl.when(goes_down(slot, j))
        def _():
            w_down(slot, j).start()

    def own_up():
        for j in range(pieces):
            if j < early:
                pass_up(co, j)
            else:
                @pl.when(jnp.logical_not(is_end))
                def _():
                    pass_up(co, j)

    for j in range(pieces):
        own_piece(j).wait()
        if j < early:
            pass_down(co, j)
        else:
            @pl.when(jnp.logical_not(is_end))
            def _():
                pass_down(co, j)
        w_mate(co, j).start()

    everything = pl.ds(0, tok)
    frequency = lax.broadcasted_iota(jnp.int32, (HD // 2, tok), 0)
    place = place_ref[...].astype(jnp.float32)
    first_end = HD // 8
    second_end = first_end + 3 * HD // 16
    chosen = jnp.where(
        frequency < first_end, place[0:1], jnp.where(frequency < second_end, place[1:2], place[2:3])
    )
    angle = chosen * freq_ref[:, 0:1]
    cos_part, sin_part = jnp.cos(angle), jnp.sin(angle)
    cosine[...] = jnp.concatenate([cos_part, cos_part], axis=0).T
    sine[...] = jnp.concatenate([-sin_part, sin_part], axis=0).T
    kvbuf[0, reach * tok:, :] = turned(k_ref[...], everything)
    kvbuf[1, reach * tok:, :] = v_ref[...]
    for part in range(2):
        kv_sends(0, part, lambda copy: copy.start())

    @pl.when(co == 0)
    def _():
        own_up()

    for d in range(reach + 1):
        @pl.when(c < d)
        def _():
            kvbuf[:, (reach - d) * tok:(reach - d + 1) * tok, :] = jnp.zeros((2, tok, HD), kvbuf.dtype)
            segments[:, (reach - d) * tok:(reach - d + 1) * tok] = jnp.full((1, tok), -1, jnp.int32)

        @pl.when(c >= d)
        def _():
            from_at = pl.multiple_of((c - d) * tok, tok)
            segments[:, (reach - d) * tok:(reach - d + 1) * tok] = segment_ref[:, pl.ds(from_at, tok)]
    own_ids = segments[:, reach * tok:].astype(jnp.float32)
    my_segment[...] = jnp.broadcast_to(own_ids, (HD, tok)).T

    def fill_bias(rt, _):
        at = pl.ds(pl.multiple_of(rt * tile, tile), tile)
        window = pl.ds(pl.multiple_of(rt * tile, tile), span)
        same = my_segment[at, 0:1] == segments[:, window].astype(jnp.float32)
        key = lax.broadcasted_iota(jnp.int32, (tile, span), 1)
        query = lax.broadcasted_iota(jnp.int32, (tile, span), 0) + reach * tok
        bias[rt] = jnp.where((key <= query) & same, 0.0, -1e30).astype(jnp.float32)
        return 0

    lax.fori_loop(0, tiles, fill_bias, 0)

    for s in range(1, stages):
        for part in (2, 3, 0, 1):
            @pl.when(co >= s)
            def _():
                landed(kv_slot(s * inner, part), kv_r.at[s * inner - 1, part])

            kv_sends(s, part, lambda copy: copy.start())
        if s == 1:
            @pl.when(co > 0)
            def _():
                own_up()

    if stages == 1:
        @pl.when(co > 0)
        def _():
            own_up()

    for d in range(1, reach + 1):
        if not chained or d % inner != 0:
            @pl.when(c >= d)
            def _():
                for part in range(kv_parts):
                    landed(kv_slot(d, part), kv_r.at[d - 1, part])

    q_copy.wait()
    residual_copy.wait()
    factor = math.log2(math.e) / math.sqrt(HD)

    def rows_of(side, at):
        return pl.ds(pl.multiple_of((side * inner + at) * quarter, quarter), quarter)

    def a_copies(hp, action):
        lanes = pl.ds(pl.multiple_of(hp * 2 * HD, 2 * HD), 2 * HD)
        for side in range(2):
            for k in range(inner):
                near = (ci + k) % inner
                for gg in range(2):
                    g = (h + gg) % 2
                    src = att.at[pl.ds(pl.multiple_of((2 * side + g) * quarter, quarter), quarter), lanes]
                    if k + gg > 0:
                        action(remote(
                            src, abuf.at[0, h, rows_of(side, ci), lanes], a_s.at[k, gg],
                            a_r.at[ci, h, side], {"ctx": co * inner + near, "tp": 2 * x + g},
                        ))

                    if k == 0:
                        @pl.when(is_end)
                        def _():
                            action(remote(
                                src, abuf.at[1, h, rows_of(side, ci), lanes], ha_s,
                                ha_r.at[ci, h, side], {"ctx": helper * inner + ci, "tp": 2 * x + g},
                            ))

    def attend(hp, _):
        lanes = pl.ds(pl.multiple_of(hp * 2 * HD, 2 * HD), 2 * HD)

        def one_tile(rt, _):
            at = pl.ds(pl.multiple_of(rt * tile, tile), tile)
            window = pl.ds(pl.multiple_of(rt * tile, tile), span)
            k = kvbuf[0, window, :]
            v = kvbuf[1, window, :]
            q2 = q_ref[at, lanes]
            done = []
            for e in range(2):
                q = turned(q2[:, e * HD:(e + 1) * HD], at)
                s = lax.dot_general(
                    q, k, (((1,), (1,)), ((), ())), preferred_element_type=jnp.float32
                ) + bias[rt]
                peak = jnp.max(s, axis=-1, keepdims=True)
                p = jnp.exp2((s - peak) * factor)
                total = jnp.sum(p, axis=-1, keepdims=True)
                mixed = jnp.dot(p.astype(jnp.bfloat16), v, preferred_element_type=jnp.float32)
                done.append((mixed / total).astype(jnp.bfloat16))
            att[at, lanes] = jnp.concatenate(done, axis=1)
            return 0

        lax.fori_loop(0, tiles, one_tile, 0)
        a_copies(hp, lambda copy: copy.start())
        for side in range(2):
            src = pl.ds(pl.multiple_of((2 * side + h) * quarter, quarter), quarter)
            abuf[0, h, rows_of(side, ci), lanes] = att[src, lanes]
        return 0

    lax.fori_loop(0, pairs, attend, 0)

    def each_side(distance, j, action):
        def one_side(side, _):
            slot = co + distance * (2 * side - 1)

            @pl.when((slot >= 0) & (slot < outer) & ((distance > 0) | (side == 1)))
            def _():
                @pl.when(has(slot, j))
                def _():
                    action(slot)
            return 0

        lax.fori_loop(0, 2, one_side, 0)

    def arrive(slot, j):
        landed(wbuf.at[slot, h, j], w_r.at[slot, h, j])
        pass_up(slot, j)
        pass_down(slot, j)
        w_mate(slot, j).start()

    def whole(slot, j):
        landed(wbuf.at[slot, 1 - h, j], w_r.at[slot, 1 - h, j])

    @pl.when(is_end)
    def _():
        for j in range(early, pieces):
            pass_up(co, j)
            pass_down(co, j)

    for j in range(early):
        each_side(1, j, lambda slot: arrive(slot, j))

    for k in range(inner):
        near = (ci + k) % inner
        for gg in range(2):
            if k + gg > 0:
                g = (h + gg) % 2
                for side in range(2):
                    landed(abuf.at[0, g, rows_of(side, near), :], a_r.at[near, g, side])

    def x_copy(who, slot, j):
        return remote(
            pbuf.at[who, slot, j, other_x], xrecv.at[who, slot, j],
            x_s.at[who, slot], x_r.at[who, slot, j], across,
        )

    def out_slot(slot, j, at):
        return out_ref.at[:, pl.ds(pl.multiple_of((slot * inner + at) * cols + j * cut, 128), cut)]

    def o_copy(who, slot, j, k):
        near = (ci + k) % inner
        node = helped if who else co
        device = {"ctx": node * inner + near, "tp": t}
        return remote(
            obuf.at[who, slot, j, near], out_slot(slot, j, ci),
            o_s.at[who, slot], o_r.at[slot, ci], device,
        )

    def plus_residual(summed, at):
        return (summed.astype(jnp.float32) + residual_ref[:, at].astype(jnp.float32)).astype(jnp.bfloat16)

    def job(who, slot, j):
        for side in range(2):
            at = slice(side * block, (side + 1) * block)
            pbuf[who, slot, j, side] = (
                jnp.dot(abuf[who, 0, at, :], wbuf[slot, 0, j], preferred_element_type=jnp.float32)
                + jnp.dot(abuf[who, 1, at, :], wbuf[slot, 1, j], preferred_element_type=jnp.float32)
            ).astype(jnp.bfloat16)
        x_copy(who, slot, j).start()

    def finish(who, slot, j):
        landed(xrecv.at[who, slot, j], x_r.at[who, slot, j])
        both = (
            pbuf[who, slot, j, x].astype(jnp.float32) + xrecv[who, slot, j].astype(jnp.float32)
        ).astype(jnp.bfloat16)
        for k in range(inner):
            obuf[who, slot, j, k] = both[k * quarter:(k + 1) * quarter]
        for k in range(1 - who, inner):
            o_copy(who, slot, j, k).start()
        if not who:
            at = pl.ds(pl.multiple_of((slot * inner + ci) * cols + j * cut, 128), cut)
            out_ref[:, at] = plus_residual(obuf[who, slot, j, ci], at)

    beyond = 2 * co - helped

    def forwards(action):
        for k in range(1, inner):
            near = (ci + k) % inner
            for g in range(2):
                for side in range(2):
                    here = abuf.at[1, g, rows_of(side, ci), :]
                    action(remote(
                        here, here, hf_s, ha_r.at[ci, g, side],
                        {"ctx": co * inner + near, "tp": t},
                    ))

    lag = min(5, pieces + 2)
    late_lag = jnp.where(2 * co >= outer, 1, 2)

    def done_by(i):
        behind = jnp.where(i < 2 * pieces, lag, late_lag)
        return jnp.clip(i - behind + 1, 0, outer * pieces)

    ahead = min(2, early)
    forward_at = max(1, min(5, pieces - 1))

    def step(i, _):
        d, j = i // pieces, i % pieces

        @pl.when((d > 1) & (d < outer))
        def _():
            each_side(d, j, lambda slot: arrive(slot, j))

        @pl.when(helps & (i == forward_at))
        def _():
            for g in range(2):
                for side in range(2):
                    landed(abuf.at[1, g, rows_of(side, ci), :], ha_r.at[ci, g, side])
            forwards(lambda copy: copy.start())

        @pl.when(helps & (i == 2 * pieces))
        def _():
            for k in range(1, inner):
                near = (ci + k) % inner
                for g in range(2):
                    for side in range(2):
                        landed(abuf.at[1, g, rows_of(side, near), :], ha_r.at[near, g, side])

            def lend(jj, _):
                job(1, beyond, jj)
                return 0

            lax.fori_loop(shared, pieces, lend, 0)

        def begins(slot):
            whole(slot, j)

            @pl.when(lends(slot, j) & (d > 1))
            def _():
                job(1, slot, j)

            job(0, slot, j)

        @pl.when(d < outer)
        def _():
            each_side(d, j, begins)

        def end_of(before, _):
            then = before % pieces

            def ends(slot):
                @pl.when(lends(slot, then) & (before >= 2 * pieces))
                def _():
                    finish(1, slot, then)

                finish(0, slot, then)

            each_side(before // pieces, then, ends)
            return 0

        lax.fori_loop(done_by(i - 1), done_by(i), end_of, 0)

        @pl.when(helps & (d == 2) & (j >= shared))
        def _():
            finish(1, beyond, j)

        @pl.when((d == 1) & (j + ahead >= early) & (j + ahead < pieces))
        def _():
            each_side(1, j, lambda slot: arrive(slot, j + ahead))
        return 0

    lax.fori_loop(0, outer * pieces + 2, step, 0)

    def kv_sent(s, k):
        landed(kvbuf.at[:, 0:tok, :], kv_s.at[s, k])

    if chained:
        for s in range(stages):
            @pl.when(co >= s)
            def _():
                if (s + 1) * inner <= reach:
                    @pl.when(co < last)
                    def _():
                        kv_sent(s, 0)
                for k in range(1, inner):
                    away = s * inner + (ci + k) % inner - ci

                    @pl.when((away >= 1) & (away <= reach))
                    def _():
                        kv_sent(s, k)
    else:
        for d in range(1, reach + 1):
            @pl.when(c + d < n)
            def _():
                kv_sent(0, d)
    for k in range(inner):
        for gg in range(2):
            if k + gg > 0:
                landed(abuf.at[0, 0, 0:2 * quarter, :], a_s.at[k, gg])

    @pl.when(is_end)
    def _():
        landed(abuf.at[0, :, 0:2 * quarter, :], ha_s)

    @pl.when(helps)
    def _():
        landed(abuf.at[1, :, 0:2 * quarter * (inner - 1), :], hf_s)

    def drain(slot, _):
        def parted(action):
            whole_unit = has(slot, pieces - 1)

            @pl.when(whole_unit)
            def _():
                action(pieces)

            if shared:
                @pl.when(has(slot, 0) & jnp.logical_not(whole_unit))
                def _():
                    action(shared)

        def sent(count):
            landed(wbuf.at[slot, h, 0:count], wm_s.at[slot])
            landed(xrecv.at[0, slot, 0:count], x_s.at[0, slot])
            landed(obuf.at[0, slot, 0:count, 0:inner - 1], o_s.at[0, slot])

        parted(sent)

        def moved(goes, sem):
            whole_unit = goes(slot, pieces - 1)

            @pl.when(whole_unit)
            def _():
                landed(wbuf.at[slot, h], sem)

            if shared:
                @pl.when(goes(slot, 0) & jnp.logical_not(whole_unit))
                def _():
                    landed(wbuf.at[slot, h, 0:shared], sem)

        moved(goes_up, wu_s.at[slot])
        moved(goes_down, wd_s.at[slot])

        def lent(start):
            landed(xrecv.at[1, slot, start:pieces], x_s.at[1, slot])
            landed(obuf.at[1, slot, start:pieces], o_s.at[1, slot])

        @pl.when(lends(slot, 0))
        def _():
            lent(0)

        if shared:
            @pl.when(lends(slot, pieces - 1) & jnp.logical_not(lends(slot, 0)))
            def _():
                lent(shared)

        return 0

    def place_of(slot, at):
        return pl.multiple_of((slot * inner + at) * cols, 128)

    def store(slot, at):
        where = pl.ds(place_of(slot, at), cols)
        return pltpu.make_async_copy(out_ref.at[:, where], result_hbm.at[:, where], out_s.at[slot, at])

    def settle(slot, at, start):
        first = pl.multiple_of(place_of(slot, at) + start * cut, 128)
        landed(out_ref.at[:, pl.ds(first, cols - start * cut)], o_r.at[slot, at])
        for j in range(start, pieces):
            where = pl.ds(pl.multiple_of(place_of(slot, at) + j * cut, 128), cut)
            out_ref[:, where] = plus_residual(out_ref[:, where], where)

    def collect(slot):
        @pl.when(jnp.logical_not(has(slot, 0)))
        def _():
            settle(slot, ci, 0)

        if shared:
            @pl.when(has(slot, 0) & jnp.logical_not(has(slot, pieces - 1)))
            def _():
                settle(slot, ci, shared)

        store(slot, ci).start()
        for k in range(1, inner):
            near = (ci + k) % inner
            settle(slot, near, 0)
            store(slot, near).start()

    def collect_at(distance, _):
        def one_side(side, _):
            slot = co + distance * (2 * side - 1)

            @pl.when((slot >= 0) & (slot < outer) & ((distance > 0) | (side == 1)))
            def _():
                collect(slot)
            return 0

        lax.fori_loop(0, 2, one_side, 0)
        return 0

    lax.fori_loop(0, outer, collect_at, 0)
    lax.fori_loop(0, outer, drain, 0)

    def stored(slot, _):
        for at in range(inner):
            store(slot, at).wait()
        return 0

    lax.fori_loop(0, outer, stored, 0)


def on_device(queries, keys, values, positions, segment_ids, out_weight, residual):
    tok = queries.shape[0]
    n = lax.axis_size("ctx")
    inner = 2 ** max(1, int(math.log2(n)) // 2)
    outer = n // inner
    reach = (DOC + tok - 2) // tok
    tile = math.gcd(tok, 256)
    depth, cols = out_weight.shape
    cut = math.gcd(cols, 128)
    pieces = cols // cut
    quarter = tok // 4
    block = inner * quarter
    bf16 = jnp.bfloat16
    dma = pltpu.SemaphoreType.DMA
    return pl.pallas_call(
        functools.partial(fused, n, inner, reach, tile),
        out_shape=jax.ShapeDtypeStruct((quarter, n * cols), bf16),
        in_specs=[pl.BlockSpec(memory_space=pltpu.HBM)] * 8,
        out_specs=pl.BlockSpec(memory_space=pltpu.HBM),
        scratch_shapes=[
            pltpu.VMEM((tok, HD), bf16),
            pltpu.VMEM((tok, HD), bf16),
            pltpu.VMEM(positions.shape, jnp.int32),
            pltpu.VMEM((1, n * tok), jnp.int32),
            pltpu.VMEM((HD // 2, HD), jnp.float32),
            pltpu.VMEM((tok, depth), bf16),
            pltpu.VMEM((quarter, n * cols), bf16),
            pltpu.VMEM((quarter, n * cols), bf16),
            pltpu.VMEM((tok, HD), jnp.float32),
            pltpu.VMEM((tok, HD), jnp.float32),
            pltpu.VMEM((tok, HD), jnp.float32),
            pltpu.VMEM((1, (reach + 1) * tok), jnp.int32),
            pltpu.VMEM((2, (reach + 1) * tok, HD), bf16),
            pltpu.VMEM((outer, 2, pieces, depth, cut), bf16),
            pltpu.VMEM((tok, depth), bf16),
            pltpu.VMEM((2, 2, 2 * block, depth), bf16),
            pltpu.VMEM((tok // tile, tile, reach * tok + tile), jnp.float32),
            pltpu.VMEM((2, outer, pieces, 2, block, cut), bf16),
            pltpu.VMEM((2, outer, pieces, block, cut), bf16),
            pltpu.VMEM((2, outer, pieces, inner, quarter, cut), bf16),
            dma((7,)), dma((outer, inner)),
            dma((reach // inner + 1, inner) if reach % inner == 0 else (1, reach + 1)), dma((reach, 4)),
            dma((outer, 2, pieces)), dma((outer,)), dma((outer,)), dma((outer,)),
            dma((inner, 2)), dma((inner, 2, 2)),
            dma, dma, dma((inner, 2, 2)),
            dma((2, outer)), dma((2, outer, pieces)),
            dma((2, outer)), dma((outer, inner)),
        ],
        compiler_params=pltpu.CompilerParams(
            collective_id=0, has_side_effects=True, vmem_limit_bytes=60 * 1024 * 1024
        ),
    )(keys, values, positions, segment_ids[None, :], half_frequencies(), queries, residual, out_weight)


def solution(mesh):
    return jax.shard_map(
        on_device,
        mesh=mesh,
        in_specs=(
            P("ctx", "tp"),
            P("ctx", "tp"),
            P("ctx", "tp"),
            P(None, "ctx"),
            P(),
            P("tp", "ctx"),
            P(("ctx", "tp"), None),
        ),
        out_specs=P(("ctx", "tp"), None),
        check_vma=False,
    )
```

```python
import functools
import math

import jax
import jax.numpy as jnp
import numpy as np
from jax import lax
from jax.experimental import pallas as pl
from jax.experimental.pallas import tpu as pltpu
from jax.sharding import PartitionSpec as P

HD = 128
DOC = 2048

theta_base = 1000000.0
MESH_ID = pl.DeviceIdType.MESH


def half_frequencies():
    index = np.arange(HD // 2, dtype=np.float64)
    values = np.power(theta_base, -2.0 * index / HD).astype(np.float32)
    return np.broadcast_to(values[:, None], (HD // 2, HD)).copy()


def fused(
    n, inner, reach, tile,
    k_hbm, v_hbm, place_hbm, segment_hbm, freq_hbm, q_hbm, residual_hbm, w_ref, result_hbm,
    k_ref, v_ref, place_ref, segment_ref, freq_ref, q_ref, residual_ref, out_ref, cosine, sine, my_segment, segments, kvbuf, wbuf, att, abuf, bias, pbuf, xrecv, obuf,
    in_s, out_s, kv_s, kv_r, w_r, wu_s, wd_s, wm_s, a_s, a_r, ha_s, hf_s, ha_r, x_s, x_r, o_s, o_r,
):
    outer = n // inner
    tok = q_ref.shape[0]
    pairs = q_ref.shape[1] // (2 * HD)
    tiles = tok // tile
    span = reach * tok + tile
    quarter = tok // 4
    pieces, cut = wbuf.shape[2], wbuf.shape[4]
    cols = w_ref.shape[1]
    block = inner * quarter
    chained = reach % inner == 0
    c = lax.axis_index("ctx")
    t = lax.axis_index("tp")
    co, ci = c // inner, c % inner
    x, h = t // 2, t % 2
    other_x = 1 - x
    last = outer - 1
    is_end = (co == 0) | (co == last)
    helps = (co == 1) | (co == last - 1)
    helped = jnp.where(co == 1, 0, last)
    helper = jnp.where(co == 0, 1, last - 1)
    mate = {"ctx": c, "tp": 2 * x + 1 - h}
    across = {"ctx": c, "tp": 2 * other_x + h}

    def remote(src, dst, send, recv, device):
        return pltpu.make_async_remote_copy(
            src_ref=src, dst_ref=dst, send_sem=send, recv_sem=recv,
            device_id=device, device_id_type=MESH_ID,
        )

    def landed(dst, sem):
        pltpu.make_async_copy(dst, dst, sem).wait()

    def own_piece(j):
        return pltpu.make_async_copy(
            w_ref.at[:, j * cut:(j + 1) * cut], wbuf.at[co, h, j], w_r.at[co, h, j]
        )

    moves = [
        pltpu.make_async_copy(src, dst, in_s.at[k]) for k, (src, dst) in enumerate([
            (place_hbm, place_ref), (freq_hbm, freq_ref), (k_hbm, k_ref), (v_hbm, v_ref),
            (segment_hbm, segment_ref), (q_hbm, q_ref), (residual_hbm, residual_ref),
        ])
    ]
    q_copy, residual_copy = moves[-2:]
    for move in moves[:-1]:
        move.start()
    for j in range(pieces):
        own_piece(j).start()

    barrier = pltpu.get_barrier_semaphore()

    def greet(device):
        pl.semaphore_signal(barrier, inc=1, device_id=device, device_id_type=MESH_ID)

    for k in range(inner):
        near = (ci + k) % inner
        for g in range(2):
            if k + g > 0:
                greet({"ctx": co * inner + near, "tp": 2 * x + (h + g) % 2})

            @pl.when(co < last)
            def _():
                greet({"ctx": (co + 1) * inner + near, "tp": 2 * x + g})

            @pl.when(co > 0)
            def _():
                greet({"ctx": (co - 1) * inner + near, "tp": 2 * x + g})
    greet(across)
    beside = jnp.where(co < last, 1, 0) + jnp.where(co > 0, 1, 0)

    def turned(vectors, at):
        wide = vectors.astype(jnp.float32)
        return (wide * cosine[at, :] + pltpu.roll(wide, HD // 2, 1) * sine[at, :]).astype(jnp.bfloat16)

    pl.semaphore_wait(barrier, 2 * inner + 2 * inner * beside)
    residual_copy.start()
    for move in moves[:-2]:
        move.wait()

    half = tok // 2
    kv_parts = 4

    def kv_slot(d, part):
        start = pl.multiple_of((reach - d) * tok + part % 2 * half, half)
        return kvbuf.at[part // 2, pl.ds(start, half), :]

    def kv_sends(s, part, action):
        src = kv_slot(s * inner, part)
        if s == 0 and part // 2 == 1:
            src = v_ref.at[pl.ds(part % 2 * half, half), :]

        def one(k, slot, device):
            action(remote(src, kv_slot(slot, part), kv_s.at[s, k], kv_r.at[slot - 1, part], device))

        if not chained:
            for d in range(1, reach + 1):
                @pl.when(c + d < n)
                def _():
                    one(d, d, {"ctx": c + d, "tp": t})
            return

        @pl.when(co >= s)
        def _():
            if (s + 1) * inner <= reach:
                @pl.when(co < last)
                def _():
                    one(0, (s + 1) * inner, {"ctx": c + inner, "tp": t})
            for k in range(1, inner):
                near = (ci + k) % inner
                away = s * inner + near - ci

                @pl.when((away >= 1) & (away <= reach))
                def _():
                    one(k, away, {"ctx": co * inner + near, "tp": t})

    stages = reach // inner + 1 if chained else 1
    for part in range(2, kv_parts):
        kv_sends(0, part, lambda copy: copy.start())

    early = (pieces + 1) // 2
    shared = pieces * 3 // 4

    def w_up(slot, j):
        device = {"ctx": c + inner, "tp": t}
        return remote(wbuf.at[slot, h, j], wbuf.at[slot, h, j], wu_s.at[slot], w_r.at[slot, h, j], device)

    def w_down(slot, j):
        device = {"ctx": c - inner, "tp": t}
        return remote(wbuf.at[slot, h, j], wbuf.at[slot, h, j], wd_s.at[slot], w_r.at[slot, h, j], device)

    def w_mate(slot, j):
        return remote(wbuf.at[slot, h, j], wbuf.at[slot, h, j], wm_s.at[slot], w_r.at[slot, h, j], mate)

    def near_end(away, j):
        return (away <= 1) | ((away == 2) & (j < shared))

    def goes_up(slot, j):
        return (slot <= co) & (co < last) & ((co + 1 < last) | near_end(co + 1 - slot, j))

    def goes_down(slot, j):
        return (slot >= co) & (co > 0) & ((co > 1) | near_end(slot - co + 1, j))

    def has(slot, j):
        return jnp.logical_not(is_end) | (near_end(slot - co, j) & near_end(co - slot, j))

    def lends(slot, j):
        away = jnp.where(slot < helped, helped - slot, slot - helped)
        return helps & jnp.logical_not(near_end(away, j))

    def pass_up(slot, j):
        @pl.when(goes_up(slot, j))
        def _():
            w_up(slot, j).start()

    def pass_down(slot, j):
        @pl.when(goes_down(slot, j))
        def _():
            w_down(slot, j).start()

    def own_up():
        for j in range(pieces):
            if j < early:
                pass_up(co, j)
            else:
                @pl.when(jnp.logical_not(is_end))
                def _():
                    pass_up(co, j)

    for j in range(pieces):
        own_piece(j).wait()
        if j < early:
            pass_down(co, j)
        else:
            @pl.when(jnp.logical_not(is_end))
            def _():
                pass_down(co, j)
        w_mate(co, j).start()

    everything = pl.ds(0, tok)
    frequency = lax.broadcasted_iota(jnp.int32, (HD // 2, tok), 0)
    place = place_ref[...].astype(jnp.float32)
    first_end = HD // 8
    second_end = first_end + 3 * HD // 16
    chosen = jnp.where(
        frequency < first_end, place[0:1], jnp.where(frequency < second_end, place[1:2], place[2:3])
    )
    angle = chosen * freq_ref[:, 0:1]
    cos_part, sin_part = jnp.cos(angle), jnp.sin(angle)
    cosine[...] = jnp.concatenate([cos_part, cos_part], axis=0).T
    sine[...] = jnp.concatenate([-sin_part, sin_part], axis=0).T
    kvbuf[0, reach * tok:, :] = turned(k_ref[...], everything)
    kvbuf[1, reach * tok:, :] = v_ref[...]
    for part in range(2):
        kv_sends(0, part, lambda copy: copy.start())

    @pl.when(co == 0)
    def _():
        own_up()

    for d in range(reach + 1):
        @pl.when(c < d)
        def _():
            kvbuf[:, (reach - d) * tok:(reach - d + 1) * tok, :] = jnp.zeros((2, tok, HD), kvbuf.dtype)
            segments[:, (reach - d) * tok:(reach - d + 1) * tok] = jnp.full((1, tok), -1, jnp.int32)

        @pl.when(c >= d)
        def _():
            from_at = pl.multiple_of((c - d) * tok, tok)
            segments[:, (reach - d) * tok:(reach - d + 1) * tok] = segment_ref[:, pl.ds(from_at, tok)]
    own_ids = segments[:, reach * tok:].astype(jnp.float32)
    my_segment[...] = jnp.broadcast_to(own_ids, (HD, tok)).T

    def fill_bias(rt, _):
        at = pl.ds(pl.multiple_of(rt * tile, tile), tile)
        window = pl.ds(pl.multiple_of(rt * tile, tile), span)
        same = my_segment[at, 0:1] == segments[:, window].astype(jnp.float32)
        key = lax.broadcasted_iota(jnp.int32, (tile, span), 1)
        query = lax.broadcasted_iota(jnp.int32, (tile, span), 0) + reach * tok
        bias[rt] = jnp.where((key <= query) & same, 0.0, -1e30).astype(jnp.float32)
        return 0

    lax.fori_loop(0, tiles, fill_bias, 0)

    for s in range(1, stages):
        for part in (2, 3, 0, 1):
            @pl.when(co >= s)
            def _():
                landed(kv_slot(s * inner, part), kv_r.at[s * inner - 1, part])

            kv_sends(s, part, lambda copy: copy.start())
        if s == 1:
            @pl.when(co > 0)
            def _():
                own_up()

    if stages == 1:
        @pl.when(co > 0)
        def _():
            own_up()

    for d in range(1, reach + 1):
        if not chained or d % inner != 0:
            @pl.when(c >= d)
            def _():
                for part in range(kv_parts):
                    landed(kv_slot(d, part), kv_r.at[d - 1, part])

    q_copy.wait()
    residual_copy.wait()
    factor = math.log2(math.e) / math.sqrt(HD)

    def rows_of(side, at):
        return pl.ds(pl.multiple_of((side * inner + at) * quarter, quarter), quarter)

    def a_copies(hp, action):
        lanes = pl.ds(pl.multiple_of(hp * 2 * HD, 2 * HD), 2 * HD)
        for side in range(2):
            for k in range(inner):
                near = (ci + k) % inner
                for gg in range(2):
                    g = (h + gg) % 2
                    src = att.at[pl.ds(pl.multiple_of((2 * side + g) * quarter, quarter), quarter), lanes]
                    if k + gg > 0:
                        action(remote(
                            src, abuf.at[0, h, rows_of(side, ci), lanes], a_s.at[k, gg],
                            a_r.at[ci, h, side], {"ctx": co * inner + near, "tp": 2 * x + g},
                        ))

                    if k == 0:
                        @pl.when(is_end)
                        def _():
                            action(remote(
                                src, abuf.at[1, h, rows_of(side, ci), lanes], ha_s,
                                ha_r.at[ci, h, side], {"ctx": helper * inner + ci, "tp": 2 * x + g},
                            ))

    def attend(hp, _):
        lanes = pl.ds(pl.multiple_of(hp * 2 * HD, 2 * HD), 2 * HD)

        def one_tile(rt, _):
            at = pl.ds(pl.multiple_of(rt * tile, tile), tile)
            window = pl.ds(pl.multiple_of(rt * tile, tile), span)
            k = kvbuf[0, window, :]
            v = kvbuf[1, window, :]
            q2 = q_ref[at, lanes]
            done = []
            for e in range(2):
                q = turned(q2[:, e * HD:(e + 1) * HD], at)
                s = lax.dot_general(
                    q, k, (((1,), (1,)), ((), ())), preferred_element_type=jnp.float32
                ) + bias[rt]
                peak = jnp.max(s, axis=-1, keepdims=True)
                p = jnp.exp2((s - peak) * factor)
                total = jnp.sum(p, axis=-1, keepdims=True)
                mixed = jnp.dot(p.astype(jnp.bfloat16), v, preferred_element_type=jnp.float32)
                done.append((mixed / total).astype(jnp.bfloat16))
            att[at, lanes] = jnp.concatenate(done, axis=1)
            return 0

        lax.fori_loop(0, tiles, one_tile, 0)
        a_copies(hp, lambda copy: copy.start())
        for side in range(2):
            src = pl.ds(pl.multiple_of((2 * side + h) * quarter, quarter), quarter)
            abuf[0, h, rows_of(side, ci), lanes] = att[src, lanes]
        return 0

    lax.fori_loop(0, pairs, attend, 0)

    def each_side(distance, j, action):
        def one_side(side, _):
            slot = co + distance * (2 * side - 1)

            @pl.when((slot >= 0) & (slot < outer) & ((distance > 0) | (side == 1)))
            def _():
                @pl.when(has(slot, j))
                def _():
                    action(slot)
            return 0

        lax.fori_loop(0, 2, one_side, 0)

    def arrive(slot, j):
        landed(wbuf.at[slot, h, j], w_r.at[slot, h, j])
        pass_up(slot, j)
        pass_down(slot, j)
        w_mate(slot, j).start()

    def whole(slot, j):
        landed(wbuf.at[slot, 1 - h, j], w_r.at[slot, 1 - h, j])

    @pl.when(is_end)
    def _():
        for j in range(early, pieces):
            pass_up(co, j)
            pass_down(co, j)

    for j in range(early):
        each_side(1, j, lambda slot: arrive(slot, j))

    for k in range(inner):
        near = (ci + k) % inner
        for gg in range(2):
            if k + gg > 0:
                g = (h + gg) % 2
                for side in range(2):
                    landed(abuf.at[0, g, rows_of(side, near), :], a_r.at[near, g, side])

    def x_copy(who, slot, j):
        return remote(
            pbuf.at[who, slot, j, other_x], xrecv.at[who, slot, j],
            x_s.at[who, slot], x_r.at[who, slot, j], across,
        )

    def out_slot(slot, j, at):
        return out_ref.at[:, pl.ds(pl.multiple_of((slot * inner + at) * cols + j * cut, 128), cut)]

    def o_copy(who, slot, j, k):
        near = (ci + k) % inner
        node = helped if who else co
        device = {"ctx": node * inner + near, "tp": t}
        return remote(
            obuf.at[who, slot, j, near], out_slot(slot, j, ci),
            o_s.at[who, slot], o_r.at[slot, ci], device,
        )

    def plus_residual(summed, at):
        return (summed.astype(jnp.float32) + residual_ref[:, at].astype(jnp.float32)).astype(jnp.bfloat16)

    def job(who, slot, j):
        for side in range(2):
            at = slice(side * block, (side + 1) * block)
            pbuf[who, slot, j, side] = (
                jnp.dot(abuf[who, 0, at, :], wbuf[slot, 0, j], preferred_element_type=jnp.float32)
                + jnp.dot(abuf[who, 1, at, :], wbuf[slot, 1, j], preferred_element_type=jnp.float32)
            ).astype(jnp.bfloat16)
        x_copy(who, slot, j).start()

    def finish(who, slot, j):
        landed(xrecv.at[who, slot, j], x_r.at[who, slot, j])
        both = (
            pbuf[who, slot, j, x].astype(jnp.float32) + xrecv[who, slot, j].astype(jnp.float32)
        ).astype(jnp.bfloat16)
        for k in range(inner):
            obuf[who, slot, j, k] = both[k * quarter:(k + 1) * quarter]
        for k in range(1 - who, inner):
            o_copy(who, slot, j, k).start()
        if not who:
            at = pl.ds(pl.multiple_of((slot * inner + ci) * cols + j * cut, 128), cut)
            out_ref[:, at] = plus_residual(obuf[who, slot, j, ci], at)

    beyond = 2 * co - helped

    def forwards(action):
        for k in range(1, inner):
            near = (ci + k) % inner
            for g in range(2):
                for side in range(2):
                    here = abuf.at[1, g, rows_of(side, ci), :]
                    action(remote(
                        here, here, hf_s, ha_r.at[ci, g, side],
                        {"ctx": co * inner + near, "tp": t},
                    ))

    lag = min(5, pieces + 2)

    def done_by(i):
        late = i - 2 * pieces
        behind = jnp.where(
            late < pieces // 4, lag, jnp.where(late < pieces // 2, 3, jnp.where(late < pieces - 1, 2, 1))
        )
        return jnp.clip(i - behind + 1, 0, outer * pieces)

    forward_at = max(1, min(5, pieces - 1))

    first = jnp.where(helps, beyond, jnp.where(co > 0, co - 1, co + 1))

    def items(i, action):
        d, j = i // pieces, i % pieces
        if pieces % 2:
            each_side(d, j, lambda slot: action(slot, j))
            return

        @pl.when(d != 1)
        def _():
            each_side(d, j, lambda slot: action(slot, j))

        slot = jnp.where(j < pieces // 2, first, 2 * co - first)

        @pl.when((d == 1) & (slot >= 0) & (slot < outer))
        def _():
            def one(m, _):
                action(slot, 2 * (j % (pieces // 2)) + m)
                return 0

            lax.fori_loop(0, 2, one, 0)

    def step(i, _):
        d, j = i // pieces, i % pieces

        @pl.when((d > 1) & (d < outer))
        def _():
            each_side(d, j, lambda slot: arrive(slot, j))

        @pl.when(helps & (i == forward_at))
        def _():
            for g in range(2):
                for side in range(2):
                    landed(abuf.at[1, g, rows_of(side, ci), :], ha_r.at[ci, g, side])
            forwards(lambda copy: copy.start())

        @pl.when(helps & (i == 2 * pieces))
        def _():
            for k in range(1, inner):
                near = (ci + k) % inner
                for g in range(2):
                    for side in range(2):
                        landed(abuf.at[1, g, rows_of(side, near), :], ha_r.at[near, g, side])

            def lend(jj, _):
                job(1, beyond, jj)
                return 0

            lax.fori_loop(shared, pieces, lend, 0)

        def begins(slot, at):
            whole(slot, at)

            @pl.when(lends(slot, at) & (d > 1))
            def _():
                job(1, slot, at)

            job(0, slot, at)

        @pl.when(d < outer)
        def _():
            items(i, begins)

        def end_of(before, _):
            def ends(slot, at):
                @pl.when(lends(slot, at) & (before >= 2 * pieces))
                def _():
                    finish(1, slot, at)

                finish(0, slot, at)

            items(before, ends)
            return 0

        lax.fori_loop(done_by(i - 1), done_by(i), end_of, 0)

        @pl.when(helps & (d == 2) & (j >= shared))
        def _():
            finish(1, beyond, j)

        @pl.when((i + 1) // pieces == 1)
        def _():
            def later(slot, at):
                @pl.when(at >= early)
                def _():
                    arrive(slot, at)

            items(i + 1, later)
        return 0

    lax.fori_loop(0, outer * pieces + 2, step, 0)

    def kv_sent(s, k):
        landed(kvbuf.at[:, 0:tok, :], kv_s.at[s, k])

    if chained:
        for s in range(stages):
            @pl.when(co >= s)
            def _():
                if (s + 1) * inner <= reach:
                    @pl.when(co < last)
                    def _():
                        kv_sent(s, 0)
                for k in range(1, inner):
                    away = s * inner + (ci + k) % inner - ci

                    @pl.when((away >= 1) & (away <= reach))
                    def _():
                        kv_sent(s, k)
    else:
        for d in range(1, reach + 1):
            @pl.when(c + d < n)
            def _():
                kv_sent(0, d)
    for k in range(inner):
        for gg in range(2):
            if k + gg > 0:
                landed(abuf.at[0, 0, 0:2 * quarter, :], a_s.at[k, gg])

    @pl.when(is_end)
    def _():
        landed(abuf.at[0, :, 0:2 * quarter, :], ha_s)

    @pl.when(helps)
    def _():
        landed(abuf.at[1, :, 0:2 * quarter * (inner - 1), :], hf_s)

    def drain(slot, _):
        def parted(action):
            whole_unit = has(slot, pieces - 1)

            @pl.when(whole_unit)
            def _():
                action(pieces)

            if shared:
                @pl.when(has(slot, 0) & jnp.logical_not(whole_unit))
                def _():
                    action(shared)

        def sent(count):
            landed(wbuf.at[slot, h, 0:count], wm_s.at[slot])
            landed(xrecv.at[0, slot, 0:count], x_s.at[0, slot])
            landed(obuf.at[0, slot, 0:count, 0:inner - 1], o_s.at[0, slot])

        parted(sent)

        def moved(goes, sem):
            whole_unit = goes(slot, pieces - 1)

            @pl.when(whole_unit)
            def _():
                landed(wbuf.at[slot, h], sem)

            if shared:
                @pl.when(goes(slot, 0) & jnp.logical_not(whole_unit))
                def _():
                    landed(wbuf.at[slot, h, 0:shared], sem)

        moved(goes_up, wu_s.at[slot])
        moved(goes_down, wd_s.at[slot])

        def lent(start):
            landed(xrecv.at[1, slot, start:pieces], x_s.at[1, slot])
            landed(obuf.at[1, slot, start:pieces], o_s.at[1, slot])

        @pl.when(lends(slot, 0))
        def _():
            lent(0)

        if shared:
            @pl.when(lends(slot, pieces - 1) & jnp.logical_not(lends(slot, 0)))
            def _():
                lent(shared)

        return 0

    def place_of(slot, at):
        return pl.multiple_of((slot * inner + at) * cols, 128)

    def store(slot, at):
        where = pl.ds(place_of(slot, at), cols)
        return pltpu.make_async_copy(out_ref.at[:, where], result_hbm.at[:, where], out_s.at[slot, at])

    def settle(slot, at, start):
        first = pl.multiple_of(place_of(slot, at) + start * cut, 128)
        landed(out_ref.at[:, pl.ds(first, cols - start * cut)], o_r.at[slot, at])
        for j in range(start, pieces):
            where = pl.ds(pl.multiple_of(place_of(slot, at) + j * cut, 128), cut)
            out_ref[:, where] = plus_residual(out_ref[:, where], where)

    def collect(slot):
        @pl.when(jnp.logical_not(has(slot, 0)))
        def _():
            settle(slot, ci, 0)

        if shared:
            @pl.when(has(slot, 0) & jnp.logical_not(has(slot, pieces - 1)))
            def _():
                settle(slot, ci, shared)

        store(slot, ci).start()
        for k in range(1, inner):
            near = (ci + k) % inner
            settle(slot, near, 0)
            store(slot, near).start()

    def collect_at(distance, _):
        def one_side(side, _):
            slot = co + distance * (2 * side - 1)

            @pl.when((slot >= 0) & (slot < outer) & ((distance > 0) | (side == 1)))
            def _():
                collect(slot)
            return 0

        lax.fori_loop(0, 2, one_side, 0)
        return 0

    lax.fori_loop(0, outer, collect_at, 0)
    lax.fori_loop(0, outer, drain, 0)

    def stored(slot, _):
        for at in range(inner):
            store(slot, at).wait()
        return 0

    lax.fori_loop(0, outer, stored, 0)


def on_device(queries, keys, values, positions, segment_ids, out_weight, residual):
    tok = queries.shape[0]
    n = lax.axis_size("ctx")
    inner = 2 ** max(1, int(math.log2(n)) // 2)
    outer = n // inner
    reach = (DOC + tok - 2) // tok
    tile = math.gcd(tok, 256)
    depth, cols = out_weight.shape
    cut = math.gcd(cols, 128)
    pieces = cols // cut
    quarter = tok // 4
    block = inner * quarter
    bf16 = jnp.bfloat16
    dma = pltpu.SemaphoreType.DMA
    return pl.pallas_call(
        functools.partial(fused, n, inner, reach, tile),
        out_shape=jax.ShapeDtypeStruct((quarter, n * cols), bf16),
        in_specs=[pl.BlockSpec(memory_space=pltpu.HBM)] * 8,
        out_specs=pl.BlockSpec(memory_space=pltpu.HBM),
        scratch_shapes=[
            pltpu.VMEM((tok, HD), bf16),
            pltpu.VMEM((tok, HD), bf16),
            pltpu.VMEM(positions.shape, jnp.int32),
            pltpu.VMEM((1, n * tok), jnp.int32),
            pltpu.VMEM((HD // 2, HD), jnp.float32),
            pltpu.VMEM((tok, depth), bf16),
            pltpu.VMEM((quarter, n * cols), bf16),
            pltpu.VMEM((quarter, n * cols), bf16),
            pltpu.VMEM((tok, HD), jnp.float32),
            pltpu.VMEM((tok, HD), jnp.float32),
            pltpu.VMEM((tok, HD), jnp.float32),
            pltpu.VMEM((1, (reach + 1) * tok), jnp.int32),
            pltpu.VMEM((2, (reach + 1) * tok, HD), bf16),
            pltpu.VMEM((outer, 2, pieces, depth, cut), bf16),
            pltpu.VMEM((tok, depth), bf16),
            pltpu.VMEM((2, 2, 2 * block, depth), bf16),
            pltpu.VMEM((tok // tile, tile, reach * tok + tile), jnp.float32),
            pltpu.VMEM((2, outer, pieces, 2, block, cut), bf16),
            pltpu.VMEM((2, outer, pieces, block, cut), bf16),
            pltpu.VMEM((2, outer, pieces, inner, quarter, cut), bf16),
            dma((7,)), dma((outer, inner)),
            dma((reach // inner + 1, inner) if reach % inner == 0 else (1, reach + 1)), dma((reach, 4)),
            dma((outer, 2, pieces)), dma((outer,)), dma((outer,)), dma((outer,)),
            dma((inner, 2)), dma((inner, 2, 2)),
            dma, dma, dma((inner, 2, 2)),
            dma((2, outer)), dma((2, outer, pieces)),
            dma((2, outer)), dma((outer, inner)),
        ],
        compiler_params=pltpu.CompilerParams(
            collective_id=0, has_side_effects=True, vmem_limit_bytes=60 * 1024 * 1024
        ),
    )(keys, values, positions, segment_ids[None, :], half_frequencies(), queries, residual, out_weight)


def solution(mesh):
    return jax.shard_map(
        on_device,
        mesh=mesh,
        in_specs=(
            P("ctx", "tp"),
            P("ctx", "tp"),
            P("ctx", "tp"),
            P(None, "ctx"),
            P(),
            P("tp", "ctx"),
            P(("ctx", "tp"), None),
        ),
        out_specs=P(("ctx", "tp"), None),
        check_vma=False,
    )
```

```python
import functools
import math

import jax
import jax.numpy as jnp
import numpy as np
from jax import lax
from jax.experimental import pallas as pl
from jax.experimental.pallas import tpu as pltpu
from jax.sharding import PartitionSpec as P

HD = 128
DOC = 2048

theta_base = 1000000.0
MESH_ID = pl.DeviceIdType.MESH


def half_frequencies():
    index = np.arange(HD // 2, dtype=np.float64)
    values = np.power(theta_base, -2.0 * index / HD).astype(np.float32)
    return np.broadcast_to(values[:, None], (HD // 2, HD)).copy()


def fused(
    n, inner, reach, tile,
    k_hbm, v_hbm, place_hbm, segment_hbm, freq_hbm, q_hbm, residual_hbm, w_ref, result_hbm,
    k_ref, v_ref, place_ref, segment_ref, freq_ref, q_ref, residual_ref, out_ref, cosine, sine, my_segment, segments, kvbuf, wbuf, att, abuf, bias, pbuf, xrecv, obuf,
    in_s, out_s, kv_s, kv_r, w_r, wu_s, wd_s, wm_s, a_s, a_r, ha_s, hf_s, ha_r, x_s, x_r, o_s, o_r,
):
    outer = n // inner
    tok = q_ref.shape[0]
    pairs = q_ref.shape[1] // (2 * HD)
    tiles = tok // tile
    span = reach * tok + tile
    quarter = tok // 4
    pieces, cut = wbuf.shape[2], wbuf.shape[4]
    cols = w_ref.shape[1]
    block = inner * quarter
    chained = reach % inner == 0
    c = lax.axis_index("ctx")
    t = lax.axis_index("tp")
    co, ci = c // inner, c % inner
    x, h = t // 2, t % 2
    other_x = 1 - x
    last = outer - 1
    is_end = (co == 0) | (co == last)
    helps = (co == 1) | (co == last - 1)
    helped = jnp.where(co == 1, 0, last)
    helper = jnp.where(co == 0, 1, last - 1)
    mate = {"ctx": c, "tp": 2 * x + 1 - h}
    across = {"ctx": c, "tp": 2 * other_x + h}

    def remote(src, dst, send, recv, device):
        return pltpu.make_async_remote_copy(
            src_ref=src, dst_ref=dst, send_sem=send, recv_sem=recv,
            device_id=device, device_id_type=MESH_ID,
        )

    def landed(dst, sem):
        pltpu.make_async_copy(dst, dst, sem).wait()

    def own_piece(j):
        return pltpu.make_async_copy(
            w_ref.at[:, j * cut:(j + 1) * cut], wbuf.at[co, h, j], w_r.at[co, h, j]
        )

    moves = [
        pltpu.make_async_copy(src, dst, in_s.at[k]) for k, (src, dst) in enumerate([
            (place_hbm, place_ref), (freq_hbm, freq_ref), (k_hbm, k_ref), (v_hbm, v_ref),
            (segment_hbm, segment_ref), (q_hbm, q_ref), (residual_hbm, residual_ref),
        ])
    ]
    q_copy, residual_copy = moves[-2:]
    for move in moves[:-1]:
        move.start()
    for j in range(pieces):
        own_piece(j).start()

    barrier = pltpu.get_barrier_semaphore()

    def greet(device):
        pl.semaphore_signal(barrier, inc=1, device_id=device, device_id_type=MESH_ID)

    for k in range(inner):
        near = (ci + k) % inner
        for g in range(2):
            if k + g > 0:
                greet({"ctx": co * inner + near, "tp": 2 * x + (h + g) % 2})

            @pl.when(co < last)
            def _():
                greet({"ctx": (co + 1) * inner + near, "tp": 2 * x + g})

            @pl.when(co > 0)
            def _():
                greet({"ctx": (co - 1) * inner + near, "tp": 2 * x + g})
    greet(across)
    beside = jnp.where(co < last, 1, 0) + jnp.where(co > 0, 1, 0)

    def turned(vectors, at):
        wide = vectors.astype(jnp.float32)
        return (wide * cosine[at, :] + pltpu.roll(wide, HD // 2, 1) * sine[at, :]).astype(jnp.bfloat16)

    pl.semaphore_wait(barrier, 2 * inner + 2 * inner * beside)
    residual_copy.start()
    for move in moves[:-2]:
        move.wait()

    half = tok // 2
    kv_parts = 4

    def kv_slot(d, part):
        start = pl.multiple_of((reach - d) * tok + part % 2 * half, half)
        return kvbuf.at[part // 2, pl.ds(start, half), :]

    def kv_sends(s, part, action):
        src = kv_slot(s * inner, part)
        if s == 0 and part // 2 == 1:
            src = v_ref.at[pl.ds(part % 2 * half, half), :]

        def one(k, slot, device):
            action(remote(src, kv_slot(slot, part), kv_s.at[s, k], kv_r.at[slot - 1, part], device))

        if not chained:
            for d in range(1, reach + 1):
                @pl.when(c + d < n)
                def _():
                    one(d, d, {"ctx": c + d, "tp": t})
            return

        @pl.when(co >= s)
        def _():
            if (s + 1) * inner <= reach:
                @pl.when(co < last)
                def _():
                    one(0, (s + 1) * inner, {"ctx": c + inner, "tp": t})
            for k in range(1, inner):
                near = (ci + k) % inner
                away = s * inner + near - ci

                @pl.when((away >= 1) & (away <= reach))
                def _():
                    one(k, away, {"ctx": co * inner + near, "tp": t})

    stages = reach // inner + 1 if chained else 1
    for part in range(2, kv_parts):
        kv_sends(0, part, lambda copy: copy.start())

    early = (pieces + 1) // 2
    shared = pieces * 7 // 8

    def w_up(slot, j):
        device = {"ctx": c + inner, "tp": t}
        return remote(wbuf.at[slot, h, j], wbuf.at[slot, h, j], wu_s.at[slot], w_r.at[slot, h, j], device)

    def w_down(slot, j):
        device = {"ctx": c - inner, "tp": t}
        return remote(wbuf.at[slot, h, j], wbuf.at[slot, h, j], wd_s.at[slot], w_r.at[slot, h, j], device)

    def w_mate(slot, j):
        return remote(wbuf.at[slot, h, j], wbuf.at[slot, h, j], wm_s.at[slot], w_r.at[slot, h, j], mate)

    def near_end(away, j):
        return (away <= 1) | ((away == 2) & (j < shared))

    def goes_up(slot, j):
        return (slot <= co) & (co < last) & ((co + 1 < last) | near_end(co + 1 - slot, j))

    def goes_down(slot, j):
        return (slot >= co) & (co > 0) & ((co > 1) | near_end(slot - co + 1, j))

    def has(slot, j):
        return jnp.logical_not(is_end) | (near_end(slot - co, j) & near_end(co - slot, j))

    def lends(slot, j):
        away = jnp.where(slot < helped, helped - slot, slot - helped)
        return helps & jnp.logical_not(near_end(away, j))

    def pass_up(slot, j):
        @pl.when(goes_up(slot, j))
        def _():
            w_up(slot, j).start()

    def pass_down(slot, j):
        @pl.when(goes_down(slot, j))
        def _():
            w_down(slot, j).start()

    def own_up():
        for j in range(pieces):
            if j < early:
                pass_up(co, j)
            else:
                @pl.when(jnp.logical_not(is_end))
                def _():
                    pass_up(co, j)

    for j in range(pieces):
        own_piece(j).wait()
        if j < early:
            pass_down(co, j)
        else:
            @pl.when(jnp.logical_not(is_end))
            def _():
                pass_down(co, j)
        w_mate(co, j).start()

    everything = pl.ds(0, tok)
    frequency = lax.broadcasted_iota(jnp.int32, (HD // 2, tok), 0)
    place = place_ref[...].astype(jnp.float32)
    first_end = HD // 8
    second_end = first_end + 3 * HD // 16
    chosen = jnp.where(
        frequency < first_end, place[0:1], jnp.where(frequency < second_end, place[1:2], place[2:3])
    )
    angle = chosen * freq_ref[:, 0:1]
    cos_part, sin_part = jnp.cos(angle), jnp.sin(angle)
    cosine[...] = jnp.concatenate([cos_part, cos_part], axis=0).T
    sine[...] = jnp.concatenate([-sin_part, sin_part], axis=0).T
    kvbuf[0, reach * tok:, :] = turned(k_ref[...], everything)
    kvbuf[1, reach * tok:, :] = v_ref[...]
    for part in range(2):
        kv_sends(0, part, lambda copy: copy.start())

    @pl.when(co == 0)
    def _():
        own_up()

    for d in range(reach + 1):
        @pl.when(c < d)
        def _():
            kvbuf[:, (reach - d) * tok:(reach - d + 1) * tok, :] = jnp.zeros((2, tok, HD), kvbuf.dtype)
            segments[:, (reach - d) * tok:(reach - d + 1) * tok] = jnp.full((1, tok), -1, jnp.int32)

        @pl.when(c >= d)
        def _():
            from_at = pl.multiple_of((c - d) * tok, tok)
            segments[:, (reach - d) * tok:(reach - d + 1) * tok] = segment_ref[:, pl.ds(from_at, tok)]
    own_ids = segments[:, reach * tok:].astype(jnp.float32)
    my_segment[...] = jnp.broadcast_to(own_ids, (HD, tok)).T

    def fill_bias(rt, _):
        at = pl.ds(pl.multiple_of(rt * tile, tile), tile)
        window = pl.ds(pl.multiple_of(rt * tile, tile), span)
        same = my_segment[at, 0:1] == segments[:, window].astype(jnp.float32)
        key = lax.broadcasted_iota(jnp.int32, (tile, span), 1)
        query = lax.broadcasted_iota(jnp.int32, (tile, span), 0) + reach * tok
        bias[rt] = jnp.where((key <= query) & same, 0.0, -1e30).astype(jnp.float32)
        return 0

    lax.fori_loop(0, tiles, fill_bias, 0)

    for s in range(1, stages):
        for part in (2, 3, 0, 1):
            @pl.when(co >= s)
            def _():
                landed(kv_slot(s * inner, part), kv_r.at[s * inner - 1, part])

            kv_sends(s, part, lambda copy: copy.start())
        if s == 1:
            @pl.when(co > 0)
            def _():
                own_up()

    if stages == 1:
        @pl.when(co > 0)
        def _():
            own_up()

    for d in range(1, reach + 1):
        if not chained or d % inner != 0:
            @pl.when(c >= d)
            def _():
                for part in range(kv_parts):
                    landed(kv_slot(d, part), kv_r.at[d - 1, part])

    q_copy.wait()
    residual_copy.wait()
    factor = math.log2(math.e) / math.sqrt(HD)

    def rows_of(side, at):
        return pl.ds(pl.multiple_of((side * inner + at) * quarter, quarter), quarter)

    def a_copies(hp, action):
        lanes = pl.ds(pl.multiple_of(hp * 2 * HD, 2 * HD), 2 * HD)
        for side in range(2):
            for k in range(inner):
                near = (ci + k) % inner
                for gg in range(2):
                    g = (h + gg) % 2
                    src = att.at[pl.ds(pl.multiple_of((2 * side + g) * quarter, quarter), quarter), lanes]
                    if k + gg > 0:
                        action(remote(
                            src, abuf.at[0, h, rows_of(side, ci), lanes], a_s.at[k, gg],
                            a_r.at[ci, h, side], {"ctx": co * inner + near, "tp": 2 * x + g},
                        ))

                    if k == 0:
                        @pl.when(is_end)
                        def _():
                            action(remote(
                                src, abuf.at[1, h, rows_of(side, ci), lanes], ha_s,
                                ha_r.at[ci, h, side], {"ctx": helper * inner + ci, "tp": 2 * x + g},
                            ))

    def attend(hp, _):
        lanes = pl.ds(pl.multiple_of(hp * 2 * HD, 2 * HD), 2 * HD)

        def one_tile(rt, _):
            at = pl.ds(pl.multiple_of(rt * tile, tile), tile)
            window = pl.ds(pl.multiple_of(rt * tile, tile), span)
            k = kvbuf[0, window, :]
            v = kvbuf[1, window, :]
            q2 = q_ref[at, lanes]
            done = []
            for e in range(2):
                q = turned(q2[:, e * HD:(e + 1) * HD], at)
                s = lax.dot_general(
                    q, k, (((1,), (1,)), ((), ())), preferred_element_type=jnp.float32
                ) + bias[rt]
                peak = jnp.max(s, axis=-1, keepdims=True)
                p = jnp.exp2((s - peak) * factor)
                total = jnp.sum(p, axis=-1, keepdims=True)
                mixed = jnp.dot(p.astype(jnp.bfloat16), v, preferred_element_type=jnp.float32)
                done.append((mixed / total).astype(jnp.bfloat16))
            att[at, lanes] = jnp.concatenate(done, axis=1)
            return 0

        lax.fori_loop(0, tiles, one_tile, 0)
        a_copies(hp, lambda copy: copy.start())
        for side in range(2):
            src = pl.ds(pl.multiple_of((2 * side + h) * quarter, quarter), quarter)
            abuf[0, h, rows_of(side, ci), lanes] = att[src, lanes]
        return 0

    lax.fori_loop(0, pairs, attend, 0)

    def each_side(distance, j, action):
        def one_side(side, _):
            slot = co + distance * (2 * side - 1)

            @pl.when((slot >= 0) & (slot < outer) & ((distance > 0) | (side == 1)))
            def _():
                @pl.when(has(slot, j))
                def _():
                    action(slot)
            return 0

        lax.fori_loop(0, 2, one_side, 0)

    def arrive(slot, j):
        landed(wbuf.at[slot, h, j], w_r.at[slot, h, j])
        pass_up(slot, j)
        pass_down(slot, j)
        w_mate(slot, j).start()

    def whole(slot, j):
        landed(wbuf.at[slot, 1 - h, j], w_r.at[slot, 1 - h, j])

    @pl.when(is_end)
    def _():
        for j in range(early, pieces):
            pass_up(co, j)
            pass_down(co, j)

    for j in range(early):
        each_side(1, j, lambda slot: arrive(slot, j))

    for k in range(inner):
        near = (ci + k) % inner
        for gg in range(2):
            if k + gg > 0:
                g = (h + gg) % 2
                for side in range(2):
                    landed(abuf.at[0, g, rows_of(side, near), :], a_r.at[near, g, side])

    def x_copy(who, slot, j):
        return remote(
            pbuf.at[who, slot, j, other_x], xrecv.at[who, slot, j],
            x_s.at[who, slot], x_r.at[who, slot, j], across,
        )

    def out_slot(slot, j, at):
        return out_ref.at[:, pl.ds(pl.multiple_of((slot * inner + at) * cols + j * cut, 128), cut)]

    def o_copy(who, slot, j, k):
        near = (ci + k) % inner
        node = helped if who else co
        device = {"ctx": node * inner + near, "tp": t}
        return remote(
            obuf.at[who, slot, j, near], out_slot(slot, j, ci),
            o_s.at[who, slot], o_r.at[slot, ci], device,
        )

    def plus_residual(summed, at):
        return (summed.astype(jnp.float32) + residual_ref[:, at].astype(jnp.float32)).astype(jnp.bfloat16)

    def job(who, slot, j):
        def one(side):
            at = pl.ds(pl.multiple_of(side * block, block), block)
            pbuf[who, slot, j, side] = (
                jnp.dot(abuf[who, 0, at, :], wbuf[slot, 0, j], preferred_element_type=jnp.float32)
                + jnp.dot(abuf[who, 1, at, :], wbuf[slot, 1, j], preferred_element_type=jnp.float32)
            ).astype(jnp.bfloat16)

        one(other_x)
        x_copy(who, slot, j).start()
        one(x)

    def finish(who, slot, j):
        landed(xrecv.at[who, slot, j], x_r.at[who, slot, j])
        both = (
            pbuf[who, slot, j, x].astype(jnp.float32) + xrecv[who, slot, j].astype(jnp.float32)
        ).astype(jnp.bfloat16)
        for k in range(inner):
            obuf[who, slot, j, k] = both[k * quarter:(k + 1) * quarter]
        for k in range(1 - who, inner):
            o_copy(who, slot, j, k).start()
        if not who:
            at = pl.ds(pl.multiple_of((slot * inner + ci) * cols + j * cut, 128), cut)
            out_ref[:, at] = plus_residual(obuf[who, slot, j, ci], at)

    beyond = 2 * co - helped

    def forwards(action):
        for k in range(1, inner):
            near = (ci + k) % inner
            for g in range(2):
                for side in range(2):
                    here = abuf.at[1, g, rows_of(side, ci), :]
                    action(remote(
                        here, here, hf_s, ha_r.at[ci, g, side],
                        {"ctx": co * inner + near, "tp": t},
                    ))

    lag = min(5, pieces + 2)

    def done_by(i):
        late = i - 2 * pieces
        behind = jnp.where(
            late < pieces // 4, lag, jnp.where(late < pieces // 2, 3, jnp.where(late < pieces - 1, 2, 1))
        )
        return jnp.clip(i - behind + 1, 0, outer * pieces)

    forward_at = max(1, min(5, pieces - 1))

    first = jnp.where(helps, beyond, jnp.where(co > 0, co - 1, co + 1))

    def items(i, action):
        d, j = i // pieces, i % pieces
        if pieces % 2:
            each_side(d, j, lambda slot: action(slot, j))
            return

        @pl.when(d != 1)
        def _():
            each_side(d, j, lambda slot: action(slot, j))

        slot = jnp.where(j < pieces // 2, first, 2 * co - first)

        @pl.when((d == 1) & (slot >= 0) & (slot < outer))
        def _():
            def one(m, _):
                action(slot, 2 * (j % (pieces // 2)) + m)
                return 0

            lax.fori_loop(0, 2, one, 0)

    def step(i, _):
        d, j = i // pieces, i % pieces

        @pl.when((d > 1) & (d < outer))
        def _():
            each_side(d, j, lambda slot: arrive(slot, j))

        @pl.when(helps & (i == forward_at))
        def _():
            for g in range(2):
                for side in range(2):
                    landed(abuf.at[1, g, rows_of(side, ci), :], ha_r.at[ci, g, side])
            forwards(lambda copy: copy.start())

        @pl.when(helps & (i == 2 * pieces))
        def _():
            for k in range(1, inner):
                near = (ci + k) % inner
                for g in range(2):
                    for side in range(2):
                        landed(abuf.at[1, g, rows_of(side, near), :], ha_r.at[near, g, side])

            def lend(jj, _):
                job(1, beyond, jj)
                return 0

            lax.fori_loop(shared, pieces, lend, 0)

        def begins(slot, at):
            whole(slot, at)

            @pl.when(lends(slot, at) & (d > 1))
            def _():
                job(1, slot, at)

            job(0, slot, at)

        @pl.when(d < outer)
        def _():
            items(i, begins)

        def end_of(before, _):
            def ends(slot, at):
                @pl.when(lends(slot, at) & (before >= 2 * pieces))
                def _():
                    finish(1, slot, at)

                finish(0, slot, at)

            items(before, ends)
            return 0

        lax.fori_loop(done_by(i - 1), done_by(i), end_of, 0)

        @pl.when(helps & (d == 2) & (j >= shared))
        def _():
            finish(1, beyond, j)

        @pl.when((i + 1) // pieces == 1)
        def _():
            def later(slot, at):
                @pl.when(at >= early)
                def _():
                    arrive(slot, at)

            items(i + 1, later)
        return 0

    lax.fori_loop(0, outer * pieces + 2, step, 0)

    def kv_sent(s, k):
        landed(kvbuf.at[:, 0:tok, :], kv_s.at[s, k])

    if chained:
        for s in range(stages):
            @pl.when(co >= s)
            def _():
                if (s + 1) * inner <= reach:
                    @pl.when(co < last)
                    def _():
                        kv_sent(s, 0)
                for k in range(1, inner):
                    away = s * inner + (ci + k) % inner - ci

                    @pl.when((away >= 1) & (away <= reach))
                    def _():
                        kv_sent(s, k)
    else:
        for d in range(1, reach + 1):
            @pl.when(c + d < n)
            def _():
                kv_sent(0, d)
    for k in range(inner):
        for gg in range(2):
            if k + gg > 0:
                landed(abuf.at[0, 0, 0:2 * quarter, :], a_s.at[k, gg])

    @pl.when(is_end)
    def _():
        landed(abuf.at[0, :, 0:2 * quarter, :], ha_s)

    @pl.when(helps)
    def _():
        landed(abuf.at[1, :, 0:2 * quarter * (inner - 1), :], hf_s)

    def drain(slot, _):
        def parted(action):
            whole_unit = has(slot, pieces - 1)

            @pl.when(whole_unit)
            def _():
                action(pieces)

            if shared:
                @pl.when(has(slot, 0) & jnp.logical_not(whole_unit))
                def _():
                    action(shared)

        def sent(count):
            landed(wbuf.at[slot, h, 0:count], wm_s.at[slot])
            landed(xrecv.at[0, slot, 0:count], x_s.at[0, slot])
            landed(obuf.at[0, slot, 0:count, 0:inner - 1], o_s.at[0, slot])

        parted(sent)

        def moved(goes, sem):
            whole_unit = goes(slot, pieces - 1)

            @pl.when(whole_unit)
            def _():
                landed(wbuf.at[slot, h], sem)

            if shared:
                @pl.when(goes(slot, 0) & jnp.logical_not(whole_unit))
                def _():
                    landed(wbuf.at[slot, h, 0:shared], sem)

        moved(goes_up, wu_s.at[slot])
        moved(goes_down, wd_s.at[slot])

        def lent(start):
            landed(xrecv.at[1, slot, start:pieces], x_s.at[1, slot])
            landed(obuf.at[1, slot, start:pieces], o_s.at[1, slot])

        @pl.when(lends(slot, 0))
        def _():
            lent(0)

        if shared:
            @pl.when(lends(slot, pieces - 1) & jnp.logical_not(lends(slot, 0)))
            def _():
                lent(shared)

        return 0

    def place_of(slot, at):
        return pl.multiple_of((slot * inner + at) * cols, 128)

    def store(slot, at):
        where = pl.ds(place_of(slot, at), cols)
        return pltpu.make_async_copy(out_ref.at[:, where], result_hbm.at[:, where], out_s)

    def settle(slot, at, start):
        first = pl.multiple_of(place_of(slot, at) + start * cut, 128)
        landed(out_ref.at[:, pl.ds(first, cols - start * cut)], o_r.at[slot, at])
        for j in range(start, pieces):
            where = pl.ds(pl.multiple_of(place_of(slot, at) + j * cut, 128), cut)
            out_ref[:, where] = plus_residual(out_ref[:, where], where)

    def collect(slot):
        @pl.when(jnp.logical_not(has(slot, 0)))
        def _():
            settle(slot, ci, 0)

        if shared:
            @pl.when(has(slot, 0) & jnp.logical_not(has(slot, pieces - 1)))
            def _():
                settle(slot, ci, shared)

        store(slot, ci).start()
        for k in range(1, inner):
            near = (ci + k) % inner
            settle(slot, near, 0)
            store(slot, near).start()

    def collect_at(distance, _):
        def one_side(side, _):
            slot = co + distance * (2 * side - 1)

            @pl.when((slot >= 0) & (slot < outer) & ((distance > 0) | (side == 1)))
            def _():
                collect(slot)
            return 0

        lax.fori_loop(0, 2, one_side, 0)
        return 0

    lax.fori_loop(0, outer, collect_at, 0)
    lax.fori_loop(0, outer, drain, 0)

    landed(out_ref, out_s)


def hand_over(parts, src, dst, held, in_s, out_s):
    rows = src.shape[0] // parts
    moves = []
    for k in range(parts):
        at = pl.ds(k * rows, rows)
        moves.append((
            pltpu.make_async_copy(src.at[at, :], held.at[at, :], in_s.at[k]),
            pltpu.make_async_copy(held.at[at, :], dst.at[at, :], out_s.at[k]),
        ))
    for take, _ in moves:
        take.start()
    for take, give in moves:
        take.wait()
        give.start()
    for _, give in moves:
        give.wait()


def on_device(queries, keys, values, positions, segment_ids, out_weight, residual):
    tok = queries.shape[0]
    n = lax.axis_size("ctx")
    inner = 2 ** max(1, int(math.log2(n)) // 2)
    outer = n // inner
    reach = (DOC + tok - 2) // tok
    tile = math.gcd(tok, 256)
    depth, cols = out_weight.shape
    cut = math.gcd(cols, 128)
    pieces = cols // cut
    quarter = tok // 4
    block = inner * quarter
    bf16 = jnp.bfloat16
    dma = pltpu.SemaphoreType.DMA
    summed = pl.pallas_call(
        functools.partial(fused, n, inner, reach, tile),
        out_shape=jax.ShapeDtypeStruct((quarter, n * cols), bf16),
        in_specs=[pl.BlockSpec(memory_space=pltpu.HBM)] * 8,
        out_specs=pl.BlockSpec(memory_space=pltpu.HBM),
        scratch_shapes=[
            pltpu.VMEM((tok, HD), bf16),
            pltpu.VMEM((tok, HD), bf16),
            pltpu.VMEM(positions.shape, jnp.int32),
            pltpu.VMEM((1, n * tok), jnp.int32),
            pltpu.VMEM((HD // 2, HD), jnp.float32),
            pltpu.VMEM((tok, depth), bf16),
            pltpu.VMEM((quarter, n * cols), bf16),
            pltpu.VMEM((quarter, n * cols), bf16),
            pltpu.VMEM((tok, HD), jnp.float32),
            pltpu.VMEM((tok, HD), jnp.float32),
            pltpu.VMEM((tok, HD), jnp.float32),
            pltpu.VMEM((1, (reach + 1) * tok), jnp.int32),
            pltpu.VMEM((2, (reach + 1) * tok, HD), bf16),
            pltpu.VMEM((outer, 2, pieces, depth, cut), bf16),
            pltpu.VMEM((tok, depth), bf16),
            pltpu.VMEM((2, 2, 2 * block, depth), bf16),
            pltpu.VMEM((tok // tile, tile, reach * tok + tile), jnp.float32),
            pltpu.VMEM((2, outer, pieces, 2, block, cut), bf16),
            pltpu.VMEM((2, outer, pieces, block, cut), bf16),
            pltpu.VMEM((2, outer, pieces, inner, quarter, cut), bf16),
            dma((7,)), dma,
            dma((reach // inner + 1, inner) if reach % inner == 0 else (1, reach + 1)), dma((reach, 4)),
            dma((outer, 2, pieces)), dma((outer,)), dma((outer,)), dma((outer,)),
            dma((inner, 2)), dma((inner, 2, 2)),
            dma, dma, dma((inner, 2, 2)),
            dma((2, outer)), dma((2, outer, pieces)),
            dma((2, outer)), dma((outer, inner)),
        ],
        compiler_params=pltpu.CompilerParams(
            collective_id=0, has_side_effects=True, vmem_limit_bytes=60 * 1024 * 1024
        ),
    )(keys, values, positions, segment_ids[None, :], half_frequencies(), queries, residual, out_weight)
    parts = math.gcd(quarter // 16, 8)
    hbm = pl.BlockSpec(memory_space=pltpu.HBM)
    return pl.pallas_call(
        functools.partial(hand_over, parts),
        out_shape=jax.ShapeDtypeStruct(summed.shape, bf16),
        in_specs=[hbm],
        out_specs=hbm,
        scratch_shapes=[pltpu.VMEM(summed.shape, bf16), dma((parts,)), dma((parts,))],
        compiler_params=pltpu.CompilerParams(vmem_limit_bytes=60 * 1024 * 1024),
    )(summed)


def solution(mesh):
    return jax.shard_map(
        on_device,
        mesh=mesh,
        in_specs=(
            P("ctx", "tp"),
            P("ctx", "tp"),
            P("ctx", "tp"),
            P(None, "ctx"),
            P(),
            P("tp", "ctx"),
            P(("ctx", "tp"), None),
        ),
        out_specs=P(("ctx", "tp"), None),
        check_vma=False,
    )
```
